32 devices in a mesh: groups: 2 (over y), dp: 4 (over z), kv: 4 (over x, core).
Axes of the slice: x: 2, y: 2, z: 4, core: 2. Of those that a mesh axis runs over, the one named last changes fastest.
Arguments:
- queries: bfloat16 [128, 3, 8192], P(('groups', 'dp'), None, 'kv'), parts along dimension 0, may hold values from -12 to 12
- routes: int32 [128, 1], P(('groups', 'dp')), parts along dimension 0, may hold values from 0 to 3; in each aligned block of 16 rows (0 to 15, 16 to 31, ...) at most 8 rows name the same one
- suffix_lengths: int32 [128], P(('groups', 'dp')), parts along dimension 0, may hold values from 128 to 256
- prefix_keys: bfloat16 [8, 2048, 1024], P(('groups', 'dp'), None, 'kv'), parts along dimension 0, may hold values from -8 to 8
- prefix_values: bfloat16 [8, 2048, 1024], P(('groups', 'dp'), None, 'kv'), parts along dimension 0, may hold values from -4.5 to 4.5
- suffix_keys: bfloat16 [128, 256, 1024], P(('groups', 'dp'), None, 'kv'), parts along dimension 0, may hold values from -4.5 to 4.5
- suffix_values: bfloat16 [128, 256, 1024], P(('groups', 'dp'), None, 'kv'), parts along dimension 0, may hold values from -4.5 to 4.5
- new_keys: bfloat16 [128, 3, 1024], P(('groups', 'dp'), None, 'kv'), parts along dimension 0, may hold values from -4.5 to 4.5
- new_values: bfloat16 [128, 3, 1024], P(('groups', 'dp'), None, 'kv'), parts along dimension 0, may hold values from -4.5 to 4.5
- out_weight: bfloat16 [8192, 8192], P('kv', 'dp'), may hold values from -0.0625 to 0.0625
Outputs:
- projected: bfloat16 [128, 3, 8192], P(('groups', 'kv'), None, 'dp'), parts along dimension 0
The draws below stay inside these ranges and needn't reach their ends.
There are 2 independent parts, one for each index of `groups`. The reference program is written for one: setup_inputs(seed, part) draws one part's arguments, and reference() takes and returns one part's arrays. A program takes and returns all parts, laid end to end along the dimension named above; an argument that names none is the same for every part. Nothing has to cross between parts.
Inputs may be any that keep to these rules, and one draw needn't show every extreme that they name: `routes`: among the 16 candidates of one index of dp at most 8 continue the same prompt, and in every draw some prompt receives exactly 8 of them from some index.
All inputs are finite; a program needn't handle non-finite values.
Results may differ from the reference program's by a relative error of at most 0.008.
Values may be sent and summed in bfloat16 or wider, within the bound.
No kernel may reach another device: no remote copies, remote signals or barrier semaphores. Data moves between devices by JAX's collectives and lax.ppermute only.
A program may use at most 128 MiB of HBM per device.

```python
import math
import jax
import jax.numpy as jnp
import numpy as np
from jax import lax

D = 8192
QHEADS = 64
KVH = 8
HD = 128
PLEN = 2048
SUF = 256
CAND_DEV = 16
STEPS = 3
PROMPTS = 4
CANDS = 64
CAP = 8


def draw_prefix_keys(key, part):
    main_key = jax.random.fold_in(key, 11)
    full_shape = (PROMPTS, PLEN, KVH * HD)
    drawn = jnp.clip(jax.random.normal(main_key, full_shape, jnp.float32), -4.5, 4.5)
    return drawn.astype(jnp.bfloat16)


def draw_suffix_keys(key, part):
    main_key = jax.random.fold_in(key, 31)
    full_shape = (CANDS, SUF, KVH * HD)
    drawn = jnp.clip(jax.random.normal(main_key, full_shape, jnp.float32), -4.5, 4.5)
    return drawn.astype(jnp.bfloat16)


def draw_queries(key, part):
    main_key = jax.random.fold_in(key, 21)
    full_shape = (CANDS, STEPS, QHEADS * HD)
    drawn = jnp.clip(3.0 * jax.random.normal(main_key, full_shape, jnp.float32), -12.0, 12.0)
    return drawn.astype(jnp.bfloat16)


def plant(result, rng, smallest, largest):
    longest = result.shape.index(max(result.shape))
    spots = []
    for shift in (0, 1):
        where = [jax.random.randint(jax.random.fold_in(rng, axis), (), 0, length) for axis, length in enumerate(result.shape)]
        where[longest] = (where[longest] + shift) % result.shape[longest]
        spots.append(tuple(where))
    return result.at[spots[0]].set(smallest).at[spots[1]].set(largest)


def shard_levels(own_key, extent, shards, low, high):
    def one(axis_at, parts):
        steps = jax.random.uniform(jax.random.fold_in(jax.random.fold_in(own_key, 6), axis_at), (parts,), jnp.float32, low / len(shards), high / len(shards))
        return jnp.repeat(jnp.exp(steps), extent[axis_at] // parts).reshape((-1,) + (1,) * (len(extent) - axis_at - 1))

    loudness = one(*shards[0])
    for cut in shards[1:]:
        loudness = loudness * one(*cut)
    return loudness


def assign_block(stream_key, own, number, rows, amount, top, limit, skew):
    order = jax.random.permutation(stream_key, amount)
    crowded, usual = load_shares(amount, rows * top, limit, skew, True), load_shares(amount, rows * top, limit, skew, False)
    places = jnp.arange(amount)

    def named(tallies, rotation):
        used = int((tallies > 0).sum())
        fixed = max(1, used // 4)
        passed = fixed + (places - fixed + rotation * (used - fixed)) % max(1, amount - fixed)
        return jnp.zeros((amount,), jnp.int32).at[order[jnp.where(places < fixed, places, passed)]].set(jnp.asarray(tallies, jnp.int32))

    tallies = jnp.where(number % 4 == 0, named(crowded, number // 4), named(usual, number - number // 4 - 1))
    mixed = jax.random.permutation(jax.random.fold_in(own, 3), amount)
    giver, receiver = mixed[0:amount // 2 * 2:2], mixed[1:amount // 2 * 2:2]
    margin = jnp.minimum(tallies[giver] - 1, limit - tallies[receiver]) // 2
    margin = jnp.where((giver == order[0]) | (receiver == order[0]) | (tallies[receiver] == 0), 0, jnp.maximum(margin, 0))
    passed = jax.random.randint(jax.random.fold_in(own, 4), (amount // 2,), 0, 1 << 20) % (margin + 1)
    tallies = tallies.at[giver].add(-passed).at[receiver].add(passed)
    members = jnp.searchsorted(jnp.cumsum(tallies), jnp.arange(rows * top), side="right").astype(jnp.int32)
    grid = members.reshape(top, rows).T
    grid = grid[jax.random.permutation(jax.random.fold_in(own, 1), rows)]
    rotation = jax.random.randint(jax.random.fold_in(own, 2), (rows, 1), 0, top)
    return jnp.take_along_axis(grid, (jnp.arange(top)[None, :] + rotation) % top, axis=1)


def load_shares(number_of, total, limit, skew, full):
    loads = [(1 << 20) // math.isqrt(rank ** skew) + 1 for rank in range(1, number_of + 1)]
    largest = limit if full else min(limit, max(-(-total // number_of), total * loads[0] // sum(loads)))
    least = 1 if total - largest >= number_of - 1 else 0
    holding, rest = [largest] + [least] * (number_of - 1), total - largest - least * (number_of - 1)
    while rest > 0:
        free = [i for i in range(1, number_of) if holding[i] < largest] or [i for i in range(1, number_of) if holding[i] < limit]
        pool, remaining = sum([loads[i] for i in free]), rest
        for i in free:
            addition = min(limit - holding[i], max(1, remaining * loads[i] // pool), rest)
            holding[i] = holding[i] + addition
            rest = rest - addition
    return np.array(holding)


def normal_values(own_key, extent, deviation, limit, split=(), kind=jnp.bfloat16):
    values = deviation * jax.random.normal(own_key, extent, jnp.float32)
    if split:
        values = values * shard_levels(own_key, extent, split, -0.22, 0.18)
    return jnp.clip(values, -limit, limit).astype(kind)


def setup_inputs(seed: int = 0, part: int = 0) -> dict:
    arg_keys = jax.random.split(jax.random.key(seed), 11)
    part_splits = jax.random.split(jax.random.fold_in(arg_keys[10], part), 11)
    queries = draw_queries(jax.random.fold_in(jax.random.fold_in(arg_keys[10], part), 71), part)
    routes_keys = jax.random.split(jax.random.fold_in(part_splits[1], 1), CANDS // CAND_DEV)
    routes_turns = jax.random.permutation(jax.random.fold_in(part_splits[1], 3), CANDS // CAND_DEV)
    routes = jax.vmap(lambda own, number: assign_block(jax.random.fold_in(part_splits[1], 2), own, number, CAND_DEV, PROMPTS, 1, CAP, 2))(routes_keys, routes_turns).reshape((CANDS, 1))
    suffix_lengths = plant(jax.random.randint(part_splits[2], (CANDS,), SUF // 2, SUF + 1), jax.random.fold_in(part_splits[2], 1), SUF // 2, SUF).astype(jnp.int32)
    prefix_keys = draw_prefix_keys(jax.random.fold_in(jax.random.fold_in(arg_keys[10], part), 71), part)
    prefix_values = normal_values(part_splits[4], (PROMPTS, PLEN, KVH * HD), 1.0, 4.5, ((0, 4), (2, 4)))
    suffix_keys = draw_suffix_keys(jax.random.fold_in(jax.random.fold_in(arg_keys[10], part), 71), part)
    suffix_values = normal_values(part_splits[6], (CANDS, SUF, KVH * HD), 1.0, 4.5, ((0, 4), (2, 4)))
    new_keys = normal_values(part_splits[7], (CANDS, STEPS, KVH * HD), 1.0, 4.5, ((0, 4), (2, 4)))
    new_values = normal_values(part_splits[8], (CANDS, STEPS, KVH * HD), 1.0, 4.5, ((0, 4), (2, 4)))
    out_weight = normal_values(arg_keys[9], (QHEADS * HD, D), (QHEADS * HD) ** -0.5, 0.0625, ((0, 4), (1, 4)))
    return {"queries": queries, "routes": routes, "suffix_lengths": suffix_lengths, "prefix_keys": prefix_keys, "prefix_values": prefix_values, "suffix_keys": suffix_keys, "suffix_values": suffix_values, "new_keys": new_keys, "new_values": new_values, "out_weight": out_weight}


def reference(queries, routes, suffix_lengths, prefix_keys, prefix_values, suffix_keys, suffix_values, new_keys, new_values, out_weight):
    group_size = QHEADS // KVH
    score_scale = 1.0 / math.sqrt(HD)
    cache_positions = jnp.arange(SUF, dtype=jnp.int32)
    step_positions = jnp.arange(STEPS, dtype=jnp.int32)
    new_allowed = step_positions[None, :] <= step_positions[:, None]

    def attend(candidate):
        query_rows, owner_index, length, cache_keys, cache_values, fresh_keys, fresh_values = candidate
        prompt_keys = lax.dynamic_index_in_dim(prefix_keys, owner_index.astype(jnp.int32), 0, keepdims=False)
        prompt_values = lax.dynamic_index_in_dim(prefix_values, owner_index.astype(jnp.int32), 0, keepdims=False)
        key_rows = jnp.concatenate([prompt_keys, cache_keys, fresh_keys], 0).astype(jnp.float32).reshape(-1, KVH, HD)
        value_rows = jnp.concatenate([prompt_values, cache_values, fresh_values], 0).astype(jnp.float32).reshape(-1, KVH, HD)
        query_heads = query_rows.astype(jnp.float32).reshape(STEPS, KVH, group_size, HD)
        scores = jnp.einsum('shgd,khd->shgk', query_heads, key_rows) * score_scale
        allowed = jnp.concatenate([jnp.ones((STEPS, PLEN), dtype=bool), jnp.broadcast_to(cache_positions[None, :] < length, (STEPS, SUF)), new_allowed], 1)
        scores = jnp.where(allowed[:, None, None, :], scores, -jnp.inf)
        peak_score = lax.optimization_barrier(jnp.max(scores, -1, keepdims=True))
        weights = jnp.exp(scores - peak_score)
        weight_sum = lax.optimization_barrier(jnp.sum(weights, -1, keepdims=True))
        combined = jnp.einsum('shgk,khd->shgd', weights / weight_sum, value_rows)
        return combined.reshape(STEPS, QHEADS * HD).astype(jnp.bfloat16)
    attended = lax.map(attend, (queries, routes[:, 0], suffix_lengths, suffix_keys, suffix_values, new_keys, new_values))
    projected = jnp.dot(attended.reshape(CANDS * STEPS, QHEADS * HD), out_weight, preferred_element_type=jnp.float32)
    return projected.reshape(CANDS, STEPS, D).astype(jnp.bfloat16)
```

```python
import functools
import math

import jax
import jax.numpy as jnp
from jax import lax
from jax.experimental import pallas as pl
from jax.experimental.pallas import tpu as pltpu
from jax.sharding import PartitionSpec as P

HD = 128
LANES = 128
F32 = jnp.float32
BF16 = jnp.bfloat16
HIDDEN = -1e30
MIB = 1 << 20
NT = (((1,), (1,)), ((), ()))


def params(mib):
    return pltpu.CompilerParams(vmem_limit_bytes=mib * MIB)


def cost(flops, nbytes, exps=0):
    return pl.CostEstimate(flops=flops, bytes_accessed=nbytes, transcendentals=exps)


def whole(count):
    return [pl.BlockSpec(memory_space=pltpu.VMEM)] * count


def slots(routes_ref, count, owners, capacity, base):
    names = [routes_ref[c] for c in range(count)]
    found = []
    for c in range(count):
        rank = jnp.int32(0)
        for earlier in range(c):
            rank = rank + (names[earlier] == names[c]).astype(jnp.int32)
        owner = names[c] - base
        owner = jnp.where(owner < 0, owner + owners, owner)
        found.append(owner * capacity + rank)
    return found


def spread(scalars, shape, dim):
    index = lax.broadcasted_iota(jnp.int32, shape, dim)
    out = jnp.full(shape, -1, jnp.int32)
    for c, value in enumerate(scalars):
        out = jnp.where(index == c, value, out)
    return out


def pack_kernel(owners, capacity, relative, routes_ref, q_ref, *out_refs):
    steps, count, _ = q_ref.shape
    base = lax.axis_index("dp") if relative else 0
    found = slots(routes_ref, count, owners, capacity, base)
    shape = (owners * capacity, count)
    placement = (spread(found, shape, 1) == lax.broadcasted_iota(jnp.int32, shape, 0)).astype(BF16)
    for s in range(steps):
        rows = jnp.dot(placement, q_ref[s], preferred_element_type=F32)
        at = 0
        for ref in out_refs:
            ref[s] = rows[at : at + ref.shape[1]].astype(BF16)
            at += ref.shape[1]


def suffix_kernel(
    group, len_ref, q_ref, k_ref, v_ref, nk_ref, nv_ref, o_ref, l_ref, qs, ss, ps, os, ls
):
    steps, count, width = q_ref.shape
    heads = width // HD // group
    cached = k_ref.shape[1]
    each = steps * group
    rows = count * each
    scale = 1.0 / math.sqrt(HD)
    to_two = scale * math.log2(math.e)
    for h in range(heads):
        for s in range(steps):
            for g in range(group):
                piece = q_ref[s, :, pl.ds((h * group + g) * HD, HD)].astype(F32)
                qs[pl.ds(h * rows + s * group + g, count, stride=each), :] = piece
    row = lax.broadcasted_iota(jnp.int32, (rows, steps * count), 0).astype(F32)
    column = lax.broadcasted_iota(jnp.int32, (rows, steps * count), 1).astype(F32)
    row_cand = jnp.floor((row + 0.5) * (1.0 / each))
    row_step = jnp.floor((row - row_cand * each + 0.5) * (1.0 / group))
    key_step = jnp.floor((column + 0.5) * (1.0 / count))
    key_cand = column - key_step * count
    visible = (row_cand == key_cand) & (key_step <= row_step)
    position = lax.broadcasted_iota(jnp.int32, (each, cached), 1)
    for h in range(heads):
        for c in range(count):
            qc = qs[pl.ds(h * rows + c * each, each), :].astype(BF16)
            kc = k_ref[c, :, pl.ds(h * HD, HD)]
            score = lax.dot_general(qc, kc, NT, preferred_element_type=F32)
            ss[pl.ds(c * each, each), :] = jnp.where(position < len_ref[c], score, HIDDEN)
        nk = jnp.concatenate([nk_ref[t, :, pl.ds(h * HD, HD)] for t in range(steps)], 0)
        nv = jnp.concatenate([nv_ref[t, :, pl.ds(h * HD, HD)] for t in range(steps)], 0)
        fresh = lax.dot_general(
            qs[pl.ds(h * rows, rows), :].astype(BF16), nk, NT, preferred_element_type=F32
        )
        fresh = jnp.where(visible, fresh, HIDDEN)
        score = ss[...]
        peak = jnp.maximum(
            jnp.max(score, -1, keepdims=True), jnp.max(fresh, -1, keepdims=True)
        )
        weight = jnp.exp2((score - peak) * to_two)
        fresh = jnp.exp2((fresh - peak) * to_two)
        total = jnp.sum(weight, -1, keepdims=True) + jnp.sum(fresh, -1, keepdims=True)
        ps[...] = weight.astype(BF16)
        os[...] = jnp.dot(fresh.astype(BF16), nv, preferred_element_type=F32)
        for c in range(count):
            vc = v_ref[c, :, pl.ds(h * HD, HD)]
            pc = ps[pl.ds(c * each, each), :]
            os[pl.ds(c * each, each), :] += jnp.dot(pc, vc, preferred_element_type=F32)
        os[...] = os[...] / total
        ls[...] = jnp.broadcast_to(peak * scale + jnp.log(total), ls.shape)
        for s in range(steps):
            for g in range(group):
                at = pl.ds(s * group + g, count, stride=each)
                lanes = pl.ds((h * group + g) * HD, HD)
                o_ref[s, :, lanes] = os[at, :]
                l_ref[s, :, lanes] = ls[at, :]


def prompt_kernel(group, blocks, *refs):
    q_refs, (k_ref, v_ref), out_refs = refs[:blocks], refs[blocks : blocks + 2], refs[blocks + 2 :]
    steps, _, width = q_refs[0].shape
    heads = width // HD // group
    all_heads = heads * group
    scale = 1.0 / math.sqrt(HD)
    to_two = scale * math.log2(math.e)
    for q_ref, out_ref in zip(q_refs, out_refs, strict=True):
        size = q_ref.shape[1]
        lane = lax.broadcasted_iota(jnp.int32, (size, LANES), 1)
        place = lax.rem(lane, all_heads)
        logs = [jnp.zeros((size, LANES), F32) for _ in range(steps)]
        for h in range(heads):
            keys = k_ref[:, pl.ds(h * HD, HD)]
            values = v_ref[:, pl.ds(h * HD, HD)]
            q = jnp.concatenate(
                [
                    q_ref[s, :, pl.ds((h * group + g) * HD, HD)]
                    for s in range(steps)
                    for g in range(group)
                ],
                0,
            )
            score = lax.dot_general(q, keys, NT, preferred_element_type=F32)
            peak = jnp.max(score, -1, keepdims=True)
            weight = jnp.exp2((score - peak) * to_two)
            total = jnp.sum(weight, -1, keepdims=True)
            out = jnp.dot(weight.astype(BF16), values, preferred_element_type=F32) / total
            log_total = peak * scale + jnp.log(total)
            for s in range(steps):
                for g in range(group):
                    at = (s * group + g) * size
                    out_ref[s, :, pl.ds((h * group + g) * HD, HD)] = out[at : at + size].astype(
                        BF16
                    )
                    logs[s] = jnp.where(
                        place == h * group + g, log_total[at : at + size], logs[s]
                    )
        for s in range(steps):
            high = logs[s].astype(BF16).astype(F32)
            rest = logs[s] - high
            middle = rest.astype(BF16).astype(F32)
            low = rest - middle
            terms = jnp.where(
                lane < all_heads, high, jnp.where(lane < 2 * all_heads, middle, low)
            )
            out_ref[s, :, pl.ds(width, LANES)] = terms.astype(BF16)


def merge_kernel(owners, capacity, relative, blocks, *refs):
    routes_ref, row_refs = refs[0], refs[1 : 1 + blocks]
    own_ref, log_ref, out_ref = refs[1 + blocks :]
    steps, count, width = own_ref.shape
    all_heads = width // HD
    base = lax.axis_index("dp") if relative else 0
    found = slots(routes_ref, count, owners, capacity, base)
    shape = (count, owners * capacity)
    choice = (spread(found, shape, 0) == lax.broadcasted_iota(jnp.int32, shape, 1)).astype(BF16)
    for s in range(steps):
        rows = jnp.concatenate([ref[s] for ref in row_refs], 0)
        rows = jnp.dot(choice, rows, preferred_element_type=F32)
        terms = rows[:, width:]
        logs = (
            terms[:, :all_heads]
            + terms[:, all_heads : 2 * all_heads]
            + terms[:, 2 * all_heads : 3 * all_heads]
        )
        for h in range(all_heads):
            lanes = slice(h * HD, (h + 1) * HD)
            first = jnp.broadcast_to(logs[:, h : h + 1], (count, HD))
            second = log_ref[s, :, lanes]
            peak = jnp.maximum(first, second)
            first = jnp.exp(first - peak)
            second = jnp.exp(second - peak)
            mixed = (first * rows[:, lanes] + second * own_ref[s, :, lanes]) / (first + second)
            out_ref[s, :, lanes] = mixed.astype(BF16)


def project_kernel(owners, parts, *refs):
    rows_refs, w_ref, own_ref, send_refs, held = (
        refs[:owners],
        refs[owners],
        refs[owners + 1],
        refs[owners + 2 : -1],
        refs[-1],
    )
    steps, count, _ = rows_refs[0].shape
    each = steps * count

    @pl.when(pl.program_id(0) == 0)
    def _():
        me, mine = lax.axis_index("dp"), lax.axis_index("kv")
        for shift, ref in enumerate(rows_refs):
            place = lax.rem(me - shift - mine + owners + parts, parts)
            for s in range(steps):
                held[place, pl.ds(s * count, count), :] = ref[s]

    product = jnp.dot(
        held[...].reshape(parts * each, held.shape[2]), w_ref[...], preferred_element_type=F32
    )
    for part, ref in enumerate((own_ref, *send_refs)):
        for s in range(steps):
            at = part * each + s * count
            ref[s] = product[at : at + count].astype(ref.dtype)


def shift_by(values, axis, amount):
    size = lax.axis_size(axis)
    return lax.ppermute(values, axis, [(i, (i + amount) % size) for i in range(size)])


def local(
    queries,
    routes,
    suffix_lengths,
    prefix_keys,
    prefix_values,
    suffix_keys,
    suffix_values,
    new_keys,
    new_values,
    out_weight,
):
    owners, parts = lax.axis_size("dp"), lax.axis_size("kv")
    count, steps, width = queries.shape
    kv_width = prefix_keys.shape[2]
    heads = kv_width // HD
    group = width // kv_width
    capacity = max(2, 2 * count // owners)
    direct = owners == parts and capacity % 8 == 0
    blocks = owners if direct else 1
    size = capacity if direct else owners * capacity
    smem = pl.BlockSpec(memory_space=pltpu.SMEM)
    q = queries.transpose(1, 0, 2)
    names = routes.reshape(count)

    packed = pl.pallas_call(
        functools.partial(pack_kernel, owners, capacity, direct),
        out_shape=[jax.ShapeDtypeStruct((steps, size, width), BF16)] * blocks,
        in_specs=[smem, *whole(1)],
        out_specs=whole(blocks),
        compiler_params=params(16),
        cost_estimate=cost(2 * steps * owners * capacity * count * width, 1 << 20),
        name="pack",
    )(names, q)

    def exchange(arrays, back):
        if direct:
            sign = -1 if back else 1
            return [arrays[0]] + [
                shift_by(values, "dp", sign * shift)
                for shift, values in enumerate(arrays)
                if shift
            ]
        values = arrays[0].reshape(steps, owners, capacity, -1)
        moved = lax.all_to_all(values, "dp", split_axis=1, concat_axis=1, tiled=True)
        return [moved.reshape(steps, owners * capacity, -1)]

    received = exchange(packed, False)

    rows = count * steps * group
    own_rows, own_logs = pl.pallas_call(
        functools.partial(suffix_kernel, group),
        out_shape=[jax.ShapeDtypeStruct((steps, count, width), F32)] * 2,
        in_specs=[smem, *whole(5)],
        out_specs=whole(2),
        scratch_shapes=[
            pltpu.VMEM((heads * rows, HD), F32),
            pltpu.VMEM((rows, suffix_keys.shape[1]), F32),
            pltpu.VMEM((rows, suffix_keys.shape[1]), BF16),
            pltpu.VMEM((rows, HD), F32),
            pltpu.VMEM((rows, LANES), F32),
        ],
        compiler_params=params(24),
        cost_estimate=cost(
            4 * heads * rows * suffix_keys.shape[1] * HD * 8, suffix_keys.size * 4, rows * 512
        ),
        name="suffix",
    )(
        suffix_lengths,
        q,
        suffix_keys,
        suffix_values,
        new_keys.transpose(1, 0, 2),
        new_values.transpose(1, 0, 2),
    )

    returned = pl.pallas_call(
        functools.partial(prompt_kernel, group, blocks),
        out_shape=[jax.ShapeDtypeStruct((steps, size, width + LANES), BF16)] * blocks,
        in_specs=whole(blocks + 2),
        out_specs=whole(blocks),
        compiler_params=params(40),
        cost_estimate=cost(
            4 * owners * capacity * steps * width * prefix_keys.shape[1], prefix_keys.size * 4
        ),
        name="prompt",
    )(*received, prefix_keys[0], prefix_values[0])
    home = exchange(returned, True)

    attended = pl.pallas_call(
        functools.partial(merge_kernel, owners, capacity, direct, blocks),
        out_shape=jax.ShapeDtypeStruct((steps, count, width), BF16),
        in_specs=[smem, *whole(blocks + 2)],
        out_specs=whole(1)[0],
        compiler_params=params(16),
        cost_estimate=cost(2 * steps * owners * capacity * count * width, 2 << 20),
        name="merge",
    )(names, *home, own_rows, own_logs)

    columns = out_weight.shape[1]
    if not direct:
        block_rows = lax.all_gather(attended, "dp", axis=1, tiled=True)
        product = jnp.dot(
            block_rows.reshape(-1, width), out_weight, preferred_element_type=F32
        ).reshape(steps, -1, columns)
        total = lax.psum_scatter(product, "kv", scatter_dimension=1, tiled=True)
        return total.astype(BF16).transpose(1, 0, 2)

    gathered = [attended] + [shift_by(attended, "dp", shift) for shift in range(1, owners)]
    chunk = columns // 4
    own_sum, *sent = pl.pallas_call(
        functools.partial(project_kernel, owners, parts),
        grid=(columns // chunk,),
        out_shape=[jax.ShapeDtypeStruct((steps, count, columns), F32)]
        + [jax.ShapeDtypeStruct((steps, count, columns), BF16)] * (parts - 1),
        in_specs=[pl.BlockSpec((steps, count, width), lambda i: (0, 0, 0))] * owners
        + [pl.BlockSpec((width, chunk), lambda i: (0, i))],
        out_specs=[pl.BlockSpec((steps, count, chunk), lambda i: (0, 0, i))] * parts,
        scratch_shapes=[pltpu.VMEM((parts, steps * count, width), BF16)],
        compiler_params=params(24),
        cost_estimate=cost(2 * owners * steps * count * width * columns, out_weight.size * 2),
        name="project",
    )(*gathered, out_weight)
    total = own_sum
    for shift, values in enumerate(sent, 1):
        total = total + shift_by(values, "kv", shift).astype(F32)
    return total.astype(BF16).transpose(1, 0, 2)


def solution(mesh):
    placed = (
        P(("groups", "dp"), None, "kv"),
        P(("groups", "dp"), None),
        P(("groups", "dp")),
        P(("groups", "dp"), None, "kv"),
        P(("groups", "dp"), None, "kv"),
        P(("groups", "dp"), None, "kv"),
        P(("groups", "dp"), None, "kv"),
        P(("groups", "dp"), None, "kv"),
        P(("groups", "dp"), None, "kv"),
        P("kv", "dp"),
    )
    return jax.shard_map(
        local,
        mesh=mesh,
        in_specs=placed,
        out_specs=P(("groups", "kv"), None, "dp"),
        check_vma=False,
    )
```

```python
import functools
import math

import jax
import jax.numpy as jnp
from jax import lax
from jax.experimental import pallas as pl
from jax.experimental.pallas import tpu as pltpu
from jax.sharding import PartitionSpec as P

HD = 128
LANES = 128
F32 = jnp.float32
BF16 = jnp.bfloat16
HIDDEN = -1e30
MIB = 1 << 20
NT = (((1,), (1,)), ((), ()))


def params(mib):
    return pltpu.CompilerParams(vmem_limit_bytes=mib * MIB)


def cost(flops, nbytes, exps=0):
    return pl.CostEstimate(flops=flops, bytes_accessed=nbytes, transcendentals=exps)


def slots(routes_ref, count, capacity, base):
    names = [routes_ref[c] for c in range(count)]
    found = []
    for c in range(count):
        rank = jnp.int32(0)
        for earlier in range(c):
            rank = rank + (names[earlier] == names[c]).astype(jnp.int32)
        found.append((names[c] ^ base) * capacity + rank)
    return found


def spread(scalars, shape, dim):
    index = lax.broadcasted_iota(jnp.int32, shape, dim)
    out = jnp.full(shape, -1, jnp.int32)
    for c, value in enumerate(scalars):
        out = jnp.where(index == c, value, out)
    return out


def pack_kernel(capacity, relative, routes_ref, q_ref, held_ref, choice_ref, *refs):
    out_refs, (names, sems) = refs[:-2], refs[-2:]
    steps, count, _ = q_ref.shape
    name_copy = pltpu.make_async_copy(routes_ref, names, sems.at[0])
    q_copy = pltpu.make_async_copy(q_ref, held_ref, sems.at[1])
    name_copy.start()
    q_copy.start()
    base = lax.axis_index("dp") if relative else 0
    name_copy.wait()
    found = slots(names, count, capacity, base)
    shape = choice_ref.shape
    choice = spread(found, shape, 0) == lax.broadcasted_iota(jnp.int32, shape, 1)
    choice_ref[...] = choice.astype(BF16)
    shape = shape[::-1]
    placement = (spread(found, shape, 1) == lax.broadcasted_iota(jnp.int32, shape, 0)).astype(BF16)
    q_copy.wait()
    for s in range(steps):
        rows = jnp.dot(placement, held_ref[s], preferred_element_type=F32)
        at = 0
        for ref in out_refs:
            ref[s] = rows[at : at + ref.shape[1]].astype(BF16)
            at += ref.shape[1]


def suffix_kernel(
    group,
    q_ref,
    len_hbm,
    k_hbm,
    v_hbm,
    nk_hbm,
    nv_hbm,
    pk_hbm,
    pv_hbm,
    o_ref,
    l_ref,
    pk_ref,
    pv_ref,
    len_ref,
    k_ref,
    v_ref,
    nk_ref,
    nv_ref,
    qs,
    ss,
    ps,
    os,
    ls,
    sems,
):
    pairs = (
        (len_hbm, len_ref),
        (k_hbm, k_ref),
        (nk_hbm, nk_ref),
        (nv_hbm, nv_ref),
        (v_hbm, v_ref),
        (pk_hbm, pk_ref),
        (pv_hbm, pv_ref),
    )
    copies = [
        pltpu.make_async_copy(source, target, sems.at[i])
        for i, (source, target) in enumerate(pairs)
    ]
    for copy in copies:
        copy.start()
    steps, count, width = q_ref.shape
    heads = width // HD // group
    cached = k_ref.shape[1]
    each = steps * group
    rows = count * each
    scale = 1.0 / math.sqrt(HD)
    to_two = scale * math.log2(math.e)
    for h in range(heads):
        for s in range(steps):
            for g in range(group):
                piece = q_ref[s, :, pl.ds((h * group + g) * HD, HD)].astype(F32)
                qs[pl.ds(h * rows + s * group + g, count, stride=each), :] = piece
    row = lax.broadcasted_iota(jnp.int32, (rows, steps * count), 0).astype(F32)
    column = lax.broadcasted_iota(jnp.int32, (rows, steps * count), 1).astype(F32)
    row_cand = jnp.floor((row + 0.5) * (1.0 / each))
    row_step = jnp.floor((row - row_cand * each + 0.5) * (1.0 / group))
    key_step = jnp.floor((column + 0.5) * (1.0 / count))
    key_cand = column - key_step * count
    visible = (row_cand == key_cand) & (key_step <= row_step)
    position = lax.broadcasted_iota(jnp.int32, (each, cached), 1)
    for copy in copies[:4]:
        copy.wait()
    for h in range(heads):
        for c in range(count):
            qc = qs[pl.ds(h * rows + c * each, each), :].astype(BF16)
            kc = k_ref[c, :, pl.ds(h * HD, HD)]
            score = lax.dot_general(qc, kc, NT, preferred_element_type=F32)
            ss[pl.ds(c * each, each), :] = jnp.where(position < len_ref[c], score, HIDDEN)
        nk = jnp.concatenate([nk_ref[t, :, pl.ds(h * HD, HD)] for t in range(steps)], 0)
        nv = jnp.concatenate([nv_ref[t, :, pl.ds(h * HD, HD)] for t in range(steps)], 0)
        fresh = lax.dot_general(
            qs[pl.ds(h * rows, rows), :].astype(BF16), nk, NT, preferred_element_type=F32
        )
        fresh = jnp.where(visible, fresh, HIDDEN)
        score = ss[...]
        peak = jnp.maximum(
            jnp.max(score, -1, keepdims=True), jnp.max(fresh, -1, keepdims=True)
        )
        weight = jnp.exp2((score - peak) * to_two)
        fresh = jnp.exp2((fresh - peak) * to_two)
        total = jnp.sum(weight, -1, keepdims=True) + jnp.sum(fresh, -1, keepdims=True)
        ps[...] = weight.astype(BF16)
        if h == 0:
            copies[4].wait()
        os[...] = jnp.dot(fresh.astype(BF16), nv, preferred_element_type=F32)
        for c in range(count):
            vc = v_ref[c, :, pl.ds(h * HD, HD)]
            pc = ps[pl.ds(c * each, each), :]
            os[pl.ds(c * each, each), :] += jnp.dot(pc, vc, preferred_element_type=F32)
        os[...] = os[...] / total
        ls[...] = jnp.broadcast_to(peak * scale + jnp.log(total), ls.shape)
        for s in range(steps):
            for g in range(group):
                at = pl.ds(s * group + g, count, stride=each)
                lanes = pl.ds((h * group + g) * HD, HD)
                o_ref[s, :, lanes] = os[at, :]
                l_ref[s, :, lanes] = ls[at, :]
    for copy in copies[5:]:
        copy.wait()


def prompt_kernel(group, q_ref, k_ref, v_ref, out_ref):
    steps, size, width = q_ref.shape
    heads = width // HD // group
    all_heads = heads * group
    scale = 1.0 / math.sqrt(HD)
    to_two = scale * math.log2(math.e)
    lane = lax.broadcasted_iota(jnp.int32, (size, LANES), 1)
    place = lax.rem(lane, all_heads)
    logs = [jnp.zeros((size, LANES), F32) for _ in range(steps)]
    for h in range(heads):
        keys = k_ref[:, pl.ds(h * HD, HD)]
        values = v_ref[:, pl.ds(h * HD, HD)]
        q = jnp.concatenate(
            [
                q_ref[s, :, pl.ds((h * group + g) * HD, HD)]
                for s in range(steps)
                for g in range(group)
            ],
            0,
        )
        score = lax.dot_general(q, keys, NT, preferred_element_type=F32)
        peak = jnp.max(score, -1, keepdims=True)
        weight = jnp.exp2((score - peak) * to_two)
        total = jnp.sum(weight, -1, keepdims=True)
        out = jnp.dot(weight.astype(BF16), values, preferred_element_type=F32) / total
        log_total = peak * scale + jnp.log(total)
        for s in range(steps):
            for g in range(group):
                at = (s * group + g) * size
                lanes = pl.ds((h * group + g) * HD, HD)
                out_ref[s, :, lanes] = out[at : at + size].astype(BF16)
                logs[s] = jnp.where(place == h * group + g, log_total[at : at + size], logs[s])
    for s in range(steps):
        high = logs[s].astype(BF16).astype(F32)
        rest = logs[s] - high
        middle = rest.astype(BF16).astype(F32)
        low = rest - middle
        terms = jnp.where(lane < all_heads, high, jnp.where(lane < 2 * all_heads, middle, low))
        out_ref[s, :, pl.ds(width, LANES)] = terms.astype(BF16)


def merge_kernel(blocks, *refs):
    choice_ref, row_refs = refs[0], refs[1 : 1 + blocks]
    own_ref, log_ref, out_ref = refs[1 + blocks :]
    steps, count, width = own_ref.shape
    all_heads = width // HD
    choice = choice_ref[...]
    for s in range(steps):
        rows = jnp.concatenate([ref[s] for ref in row_refs], 0)
        rows = jnp.dot(choice, rows, preferred_element_type=F32)
        terms = rows[:, width:]
        logs = (
            terms[:, :all_heads]
            + terms[:, all_heads : 2 * all_heads]
            + terms[:, 2 * all_heads : 3 * all_heads]
        )
        for h in range(all_heads):
            lanes = slice(h * HD, (h + 1) * HD)
            first = jnp.broadcast_to(logs[:, h : h + 1], (count, HD))
            second = log_ref[s, :, lanes]
            peak = jnp.maximum(first, second)
            first = jnp.exp(first - peak)
            second = jnp.exp(second - peak)
            mixed = (first * rows[:, lanes] + second * own_ref[s, :, lanes]) / (first + second)
            out_ref[s, :, lanes] = mixed.astype(BF16)


def project_kernel(owners, parts, *refs):
    rows_refs, w_ref, own_ref, send_refs, held = (
        refs[:owners],
        refs[owners],
        refs[owners + 1],
        refs[owners + 2 : -1],
        refs[-1],
    )
    steps, count, _ = rows_refs[0].shape
    each = steps * count

    @pl.when(pl.program_id(0) == 0)
    def _():
        me, mine = lax.axis_index("dp"), lax.axis_index("kv")
        for shift, ref in enumerate(rows_refs):
            place = (me ^ shift) ^ mine
            for s in range(steps):
                held[place, pl.ds(s * count, count), :] = ref[s]

    product = jnp.dot(
        held[...].reshape(parts * each, held.shape[2]), w_ref[...], preferred_element_type=F32
    )
    for part, ref in enumerate((own_ref, *send_refs)):
        for s in range(steps):
            at = part * each + s * count
            ref[s] = product[at : at + count].astype(ref.dtype)


def swap(values, axis, mask):
    return lax.ppermute(values, axis, [(i, i ^ mask) for i in range(lax.axis_size(axis))])


def local(
    queries,
    routes,
    suffix_lengths,
    prefix_keys,
    prefix_values,
    suffix_keys,
    suffix_values,
    new_keys,
    new_values,
    out_weight,
):
    owners, parts = lax.axis_size("dp"), lax.axis_size("kv")
    count, steps, width = queries.shape
    kv_width = prefix_keys.shape[2]
    heads = kv_width // HD
    group = width // kv_width
    capacity = max(2, 2 * count // owners)
    direct = owners == parts == 4 and capacity % 8 == 0
    blocks = owners if direct else 1
    size = capacity if direct else owners * capacity
    vmem, hbm = pl.BlockSpec(memory_space=pltpu.VMEM), pl.BlockSpec(memory_space=pltpu.HBM)
    far = lambda values: pltpu.with_memory_space_constraint(values, pltpu.HBM)
    names = routes.reshape(count)

    q, choice, *packed = pl.pallas_call(
        functools.partial(pack_kernel, capacity, direct),
        out_shape=[
            jax.ShapeDtypeStruct((steps, count, width), BF16),
            jax.ShapeDtypeStruct((count, owners * capacity), BF16),
        ]
        + [jax.ShapeDtypeStruct((steps, size, width), BF16)] * blocks,
        in_specs=[hbm, hbm],
        out_specs=[vmem] * (blocks + 2),
        scratch_shapes=[pltpu.SMEM((count,), jnp.int32), pltpu.SemaphoreType.DMA((2,))],
        compiler_params=params(8),
        cost_estimate=cost(2 * steps * owners * capacity * count * width, 1 << 20),
        name="pack",
    )(far(names), far(queries.transpose(1, 0, 2)))

    def all_to_all(values):
        values = values.reshape(steps, owners, capacity, -1)
        moved = lax.all_to_all(values, "dp", split_axis=1, concat_axis=1, tiled=True)
        return moved.reshape(steps, owners * capacity, -1)

    if direct:
        received = [packed[0]] + [swap(packed[mask], "dp", mask) for mask in (1, 2, 3)]
    else:
        received = [all_to_all(packed[0])]

    rows = count * steps * group
    cached = suffix_keys.shape[1]
    new_shape = (steps, count, kv_width)
    own_rows, own_logs, keys, values = pl.pallas_call(
        functools.partial(suffix_kernel, group),
        out_shape=[jax.ShapeDtypeStruct((steps, count, width), F32)] * 2
        + [jax.ShapeDtypeStruct(prefix_keys.shape[1:], BF16)] * 2,
        in_specs=[vmem] + [hbm] * 7,
        out_specs=[vmem] * 4,
        scratch_shapes=[
            pltpu.SMEM((count,), jnp.int32),
            pltpu.VMEM(suffix_keys.shape, BF16),
            pltpu.VMEM(suffix_keys.shape, BF16),
            pltpu.VMEM(new_shape, BF16),
            pltpu.VMEM(new_shape, BF16),
            pltpu.VMEM((heads * rows, HD), F32),
            pltpu.VMEM((rows, cached), F32),
            pltpu.VMEM((rows, cached), BF16),
            pltpu.VMEM((rows, HD), F32),
            pltpu.VMEM((rows, LANES), F32),
            pltpu.SemaphoreType.DMA((7,)),
        ],
        compiler_params=params(16),
        cost_estimate=cost(3_000_000_000, suffix_keys.size * 4, rows * 512),
        name="suffix",
    )(
        q,
        far(suffix_lengths),
        far(suffix_keys),
        far(suffix_values),
        far(new_keys.transpose(1, 0, 2)),
        far(new_values.transpose(1, 0, 2)),
        far(prefix_keys[0]),
        far(prefix_values[0]),
    )

    prompt = pl.pallas_call(
        functools.partial(prompt_kernel, group),
        out_shape=jax.ShapeDtypeStruct((steps, size, width + LANES), BF16),
        in_specs=[vmem] * 3,
        out_specs=vmem,
        compiler_params=params(12 if direct else 48),
        cost_estimate=cost(4 * size * steps * width * prefix_keys.shape[1], prefix_keys.size * 4),
        name="prompt",
    )
    answers = [prompt(block, keys, values) for block in received]
    if direct:
        home = [answers[0]] + [swap(answers[mask], "dp", mask) for mask in (1, 2, 3)]
    else:
        home = [all_to_all(answers[0])]

    attended = pl.pallas_call(
        functools.partial(merge_kernel, blocks),
        out_shape=jax.ShapeDtypeStruct((steps, count, width), BF16),
        in_specs=[vmem] * (blocks + 3),
        out_specs=vmem,
        compiler_params=params(8),
        cost_estimate=cost(2 * steps * owners * capacity * count * width, 2 << 20),
        name="merge",
    )(choice, *home, own_rows, own_logs)

    columns = out_weight.shape[1]
    if not direct:
        block_rows = lax.all_gather(attended, "dp", axis=1, tiled=True)
        product = jnp.dot(
            block_rows.reshape(-1, width), out_weight, preferred_element_type=F32
        ).reshape(steps, -1, columns)
        total = lax.psum_scatter(product, "kv", scatter_dimension=1, tiled=True)
        return total.astype(BF16).transpose(1, 0, 2)

    gathered = [attended] + [swap(attended, "dp", mask) for mask in (1, 2, 3)]
    chunk = columns // 4
    own_sum, *sent = pl.pallas_call(
        functools.partial(project_kernel, owners, parts),
        grid=(columns // chunk,),
        out_shape=[jax.ShapeDtypeStruct((steps, count, columns), F32)]
        + [jax.ShapeDtypeStruct((steps, count, columns), BF16)] * (parts - 1),
        in_specs=[pl.BlockSpec((steps, count, width), lambda i: (0, 0, 0))] * owners
        + [pl.BlockSpec((width, chunk), lambda i: (0, i))],
        out_specs=[pl.BlockSpec((steps, count, chunk), lambda i: (0, 0, i))] * parts,
        scratch_shapes=[pltpu.VMEM((parts, steps * count, width), BF16)],
        compiler_params=params(24),
        cost_estimate=cost(2 * owners * steps * count * width * columns, out_weight.size * 2),
        name="project",
    )(*gathered, out_weight)
    total = own_sum
    for shift, values in enumerate(sent, 1):
        total = total + swap(values, "kv", shift).astype(F32)
    return total.astype(BF16).transpose(1, 0, 2)


def solution(mesh):
    placed = (
        P(("groups", "dp"), None, "kv"),
        P(("groups", "dp"), None),
        P(("groups", "dp")),
        P(("groups", "dp"), None, "kv"),
        P(("groups", "dp"), None, "kv"),
        P(("groups", "dp"), None, "kv"),
        P(("groups", "dp"), None, "kv"),
        P(("groups", "dp"), None, "kv"),
        P(("groups", "dp"), None, "kv"),
        P("kv", "dp"),
    )
    return jax.shard_map(
        local,
        mesh=mesh,
        in_specs=placed,
        out_specs=P(("groups", "kv"), None, "dp"),
        check_vma=False,
    )
```

```python
import functools
import math

import jax
import jax.numpy as jnp
from jax import lax
from jax.experimental import pallas as pl
from jax.experimental.pallas import tpu as pltpu
from jax.sharding import PartitionSpec as P


HD = 128
LANES = 128
F32 = jnp.float32
BF16 = jnp.bfloat16
HIDDEN = -1e30
MIB = 1 << 20
NT = (((1,), (1,)), ((), ()))


def params(mib):
    return pltpu.CompilerParams(vmem_limit_bytes=mib * MIB)


def cost(flops, nbytes, exps=0):
    return pl.CostEstimate(flops=flops, bytes_accessed=nbytes, transcendentals=exps)


def slots(routes_ref, count, capacity, base):
    names = [routes_ref[c] for c in range(count)]
    found = []
    for c in range(count):
        rank = jnp.int32(0)
        for earlier in range(c):
            rank = rank + (names[earlier] == names[c]).astype(jnp.int32)
        found.append((names[c] ^ base) * capacity + rank)
    return found


def spread(scalars, shape, dim):
    index = lax.broadcasted_iota(jnp.int32, shape, dim)
    out = jnp.full(shape, -1, jnp.int32)
    for c, value in enumerate(scalars):
        out = jnp.where(index == c, value, out)
    return out


def pack_kernel(capacity, relative, routes_ref, q_ref, held_ref, choice_ref, *refs):
    out_refs, (names, sems) = refs[:-2], refs[-2:]
    steps, count, _ = q_ref.shape
    name_copy = pltpu.make_async_copy(routes_ref, names, sems.at[0])
    q_copy = pltpu.make_async_copy(q_ref, held_ref, sems.at[1])
    name_copy.start()
    q_copy.start()
    base = lax.axis_index("dp") if relative else 0
    name_copy.wait()
    found = slots(names, count, capacity, base)
    shape = choice_ref.shape
    choice = spread(found, shape, 0) == lax.broadcasted_iota(jnp.int32, shape, 1)
    choice_ref[...] = choice.astype(BF16)
    shape = shape[::-1]
    placement = (spread(found, shape, 1) == lax.broadcasted_iota(jnp.int32, shape, 0)).astype(BF16)
    q_copy.wait()
    for s in range(steps):
        rows = jnp.dot(placement, held_ref[s], preferred_element_type=F32)
        at = 0
        for ref in out_refs:
            ref[s] = rows[at : at + ref.shape[1]].astype(BF16)
            at += ref.shape[1]


def suffix_kernel(
    group,
    q_ref,
    len_hbm,
    k_hbm,
    v_hbm,
    nk_hbm,
    nv_hbm,
    pk_hbm,
    pv_hbm,
    o_ref,
    l_ref,
    pk_ref,
    pv_ref,
    len_ref,
    k_ref,
    v_ref,
    nk_ref,
    nv_ref,
    qs,
    ss,
    ps,
    os,
    ls,
    sems,
):
    pairs = (
        (len_hbm, len_ref),
        (k_hbm, k_ref),
        (nk_hbm, nk_ref),
        (nv_hbm, nv_ref),
        (v_hbm, v_ref),
        (pk_hbm, pk_ref),
        (pv_hbm, pv_ref),
    )
    copies = [
        pltpu.make_async_copy(source, target, sems.at[i])
        for i, (source, target) in enumerate(pairs)
    ]
    for copy in copies:
        copy.start()
    steps, count, width = q_ref.shape
    heads = width // HD // group
    cached = k_ref.shape[1]
    each = steps * group
    rows = count * each
    scale = 1.0 / math.sqrt(HD)
    to_two = scale * math.log2(math.e)
    for h in range(heads):
        for s in range(steps):
            for g in range(group):
                piece = q_ref[s, :, pl.ds((h * group + g) * HD, HD)].astype(F32)
                qs[pl.ds(h * rows + s * group + g, count, stride=each), :] = piece
    row = lax.broadcasted_iota(jnp.int32, (rows, steps * count), 0).astype(F32)
    column = lax.broadcasted_iota(jnp.int32, (rows, steps * count), 1).astype(F32)
    row_cand = jnp.floor((row + 0.5) * (1.0 / each))
    row_step = jnp.floor((row - row_cand * each + 0.5) * (1.0 / group))
    key_step = jnp.floor((column + 0.5) * (1.0 / count))
    key_cand = column - key_step * count
    visible = (row_cand == key_cand) & (key_step <= row_step)
    position = lax.broadcasted_iota(jnp.int32, (each, cached), 1)
    for copy in copies[:4]:
        copy.wait()
    for h in range(heads):
        for c in range(count):
            qc = qs[pl.ds(h * rows + c * each, each), :].astype(BF16)
            kc = k_ref[c, :, pl.ds(h * HD, HD)]
            score = lax.dot_general(qc, kc, NT, preferred_element_type=F32)
            ss[pl.ds(c * each, each), :] = jnp.where(position < len_ref[c], score, HIDDEN)
        nk = jnp.concatenate([nk_ref[t, :, pl.ds(h * HD, HD)] for t in range(steps)], 0)
        nv = jnp.concatenate([nv_ref[t, :, pl.ds(h * HD, HD)] for t in range(steps)], 0)
        fresh = lax.dot_general(
            qs[pl.ds(h * rows, rows), :].astype(BF16), nk, NT, preferred_element_type=F32
        )
        fresh = jnp.where(visible, fresh, HIDDEN)
        score = ss[...]
        peak = jnp.maximum(
            jnp.max(score, -1, keepdims=True), jnp.max(fresh, -1, keepdims=True)
        )
        weight = jnp.exp2((score - peak) * to_two)
        fresh = jnp.exp2((fresh - peak) * to_two)
        total = jnp.sum(weight, -1, keepdims=True) + jnp.sum(fresh, -1, keepdims=True)
        ps[...] = weight.astype(BF16)
        if h == 0:
            copies[4].wait()
        os[...] = jnp.dot(fresh.astype(BF16), nv, preferred_element_type=F32)
        for c in range(count):
            vc = v_ref[c, :, pl.ds(h * HD, HD)]
            pc = ps[pl.ds(c * each, each), :]
            os[pl.ds(c * each, each), :] += jnp.dot(pc, vc, preferred_element_type=F32)
        os[...] = os[...] / total
        ls[...] = jnp.broadcast_to(peak * scale + jnp.log(total), ls.shape)
        for s in range(steps):
            for g in range(group):
                at = pl.ds(s * group + g, count, stride=each)
                lanes = pl.ds((h * group + g) * HD, HD)
                o_ref[s, :, lanes] = os[at, :]
                l_ref[s, :, lanes] = ls[at, :]
    for copy in copies[5:]:
        copy.wait()


def prompt_kernel(group, q_ref, k_ref, v_ref, out_ref):
    steps, size, width = q_ref.shape
    heads = width // HD // group
    all_heads = heads * group
    scale = 1.0 / math.sqrt(HD)
    to_two = scale * math.log2(math.e)
    lane = lax.broadcasted_iota(jnp.int32, (size, LANES), 1)
    place = lax.rem(lane, all_heads)
    logs = [jnp.zeros((size, LANES), F32) for _ in range(steps)]
    for h in range(heads):
        keys = k_ref[:, pl.ds(h * HD, HD)]
        values = v_ref[:, pl.ds(h * HD, HD)]
        q = jnp.concatenate(
            [
                q_ref[s, :, pl.ds((h * group + g) * HD, HD)]
                for s in range(steps)
                for g in range(group)
            ],
            0,
        )
        score = lax.dot_general(q, keys, NT, preferred_element_type=F32)
        peak = jnp.max(score, -1, keepdims=True)
        weight = jnp.exp2((score - peak) * to_two)
        total = jnp.sum(weight, -1, keepdims=True)
        out = jnp.dot(weight.astype(BF16), values, preferred_element_type=F32) / total
        log_total = peak * scale + jnp.log(total)
        for s in range(steps):
            for g in range(group):
                at = (s * group + g) * size
                lanes = pl.ds((h * group + g) * HD, HD)
                out_ref[s, :, lanes] = out[at : at + size].astype(BF16)
                logs[s] = jnp.where(place == h * group + g, log_total[at : at + size], logs[s])
    for s in range(steps):
        high = logs[s].astype(BF16).astype(F32)
        rest = logs[s] - high
        middle = rest.astype(BF16).astype(F32)
        low = rest - middle
        terms = jnp.where(lane < all_heads, high, jnp.where(lane < 2 * all_heads, middle, low))
        out_ref[s, :, pl.ds(width, LANES)] = terms.astype(BF16)


def merge_kernel(blocks, *refs):
    choice_ref, row_refs = refs[0], refs[1 : 1 + blocks]
    own_ref, log_ref, out_ref = refs[1 + blocks :]
    steps, count, width = own_ref.shape
    all_heads = width // HD
    choice = choice_ref[...]
    for s in range(steps):
        rows = jnp.concatenate([ref[s] for ref in row_refs], 0)
        rows = jnp.dot(choice, rows, preferred_element_type=F32)
        terms = rows[:, width:]
        logs = (
            terms[:, :all_heads]
            + terms[:, all_heads : 2 * all_heads]
            + terms[:, 2 * all_heads : 3 * all_heads]
        )
        for h in range(all_heads):
            lanes = slice(h * HD, (h + 1) * HD)
            first = jnp.broadcast_to(logs[:, h : h + 1], (count, HD))
            second = log_ref[s, :, lanes]
            peak = jnp.maximum(first, second)
            first = jnp.exp(first - peak)
            second = jnp.exp(second - peak)
            mixed = (first * rows[:, lanes] + second * own_ref[s, :, lanes]) / (first + second)
            out_ref[s, :, lanes] = mixed.astype(BF16)


def project_kernel(shifts, *refs):
    *rows_refs, w_ref, keep_ref, send_ref, held = refs
    steps, count, _ = keep_ref.shape
    each = steps * count

    @pl.when(pl.program_id(0) == 0)
    def _():
        me, mine = lax.axis_index("dp"), lax.axis_index("kv")
        inner = (me == 1) | (me == 2)
        for at, shift in enumerate(shifts):
            place = ((me ^ shift) ^ mine) & 1
            choices = rows_refs[2 * at : 2 * at + 2] if len(rows_refs) > 2 else rows_refs[at:at + 1]
            if len(choices) == 1:
                for s in range(steps):
                    held[place, pl.ds(s * count, count), :] = choices[0][s]
            else:

                @pl.when(inner)
                def _():
                    for s in range(steps):
                        held[place, pl.ds(s * count, count), :] = choices[0][s]

                @pl.when(jnp.logical_not(inner))
                def _():
                    for s in range(steps):
                        held[place, pl.ds(s * count, count), :] = choices[1][s]

    product = jnp.dot(
        held[...].reshape(2 * each, held.shape[2]), w_ref[...], preferred_element_type=F32
    )
    for part, ref in enumerate((keep_ref, send_ref)):
        for s in range(steps):
            at = part * each + s * count
            ref[s] = product[at : at + count].astype(ref.dtype)


def add_kernel(keep_ref, got_ref, sum_ref, send_ref):
    for s in range(keep_ref.shape[0]):
        total = keep_ref[s] + got_ref[s].astype(F32)
        sum_ref[s] = total
        send_ref[s] = total.astype(BF16)


def swap(values, axis, mask):
    pairs = [(i, i ^ mask) for i in range(lax.axis_size(axis))]
    return lax.ppermute(values, axis, pairs)


def local(
    queries,
    routes,
    suffix_lengths,
    prefix_keys,
    prefix_values,
    suffix_keys,
    suffix_values,
    new_keys,
    new_values,
    out_weight,
):
    owners, parts = lax.axis_size("dp"), lax.axis_size("kv")
    count, steps, width = queries.shape
    kv_width = prefix_keys.shape[2]
    heads = kv_width // HD
    group = width // kv_width
    capacity = max(2, 2 * count // owners)
    direct = owners == parts == 4 and capacity % 8 == 0
    blocks = owners if direct else 1
    size = capacity if direct else owners * capacity
    vmem, hbm = pl.BlockSpec(memory_space=pltpu.VMEM), pl.BlockSpec(memory_space=pltpu.HBM)
    far = lambda values: pltpu.with_memory_space_constraint(values, pltpu.HBM)
    names = routes.reshape(count)

    q, choice, *packed = pl.pallas_call(
        functools.partial(pack_kernel, capacity, direct),
        out_shape=[
            jax.ShapeDtypeStruct((steps, count, width), BF16),
            jax.ShapeDtypeStruct((count, owners * capacity), BF16),
        ]
        + [jax.ShapeDtypeStruct((steps, size, width), BF16)] * blocks,
        in_specs=[hbm, hbm],
        out_specs=[vmem] * (blocks + 2),
        scratch_shapes=[pltpu.SMEM((count,), jnp.int32), pltpu.SemaphoreType.DMA((2,))],
        compiler_params=params(8),
        cost_estimate=cost(2 * steps * owners * capacity * count * width, 1 << 20),
        name="pack",
    )(far(names), far(queries.transpose(1, 0, 2)))

    def all_to_all(values):
        values = values.reshape(steps, owners, capacity, -1)
        moved = lax.all_to_all(values, "dp", split_axis=1, concat_axis=1, tiled=True)
        return moved.reshape(steps, owners * capacity, -1)

    if direct:
        received = [packed[0]] + [swap(packed[i], "dp", i) for i in (1, 2, 3)]
    else:
        received = [all_to_all(packed[0])]

    rows = count * steps * group
    cached = suffix_keys.shape[1]
    new_shape = (steps, count, kv_width)
    own_rows, own_logs, keys, values = pl.pallas_call(
        functools.partial(suffix_kernel, group),
        out_shape=[jax.ShapeDtypeStruct((steps, count, width), F32)] * 2
        + [jax.ShapeDtypeStruct(prefix_keys.shape[1:], BF16)] * 2,
        in_specs=[vmem] + [hbm] * 7,
        out_specs=[vmem] * 4,
        scratch_shapes=[
            pltpu.SMEM((count,), jnp.int32),
            pltpu.VMEM(suffix_keys.shape, BF16),
            pltpu.VMEM(suffix_keys.shape, BF16),
            pltpu.VMEM(new_shape, BF16),
            pltpu.VMEM(new_shape, BF16),
            pltpu.VMEM((heads * rows, HD), F32),
            pltpu.VMEM((rows, cached), F32),
            pltpu.VMEM((rows, cached), BF16),
            pltpu.VMEM((rows, HD), F32),
            pltpu.VMEM((rows, LANES), F32),
            pltpu.SemaphoreType.DMA((7,)),
        ],
        compiler_params=params(16),
        cost_estimate=cost(3_000_000_000, suffix_keys.size * 4, rows * 512),
        name="suffix",
    )(
        q,
        far(suffix_lengths),
        far(suffix_keys),
        far(suffix_values),
        far(new_keys.transpose(1, 0, 2)),
        far(new_values.transpose(1, 0, 2)),
        far(prefix_keys[0]),
        far(prefix_values[0]),
    )

    prompt = pl.pallas_call(
        functools.partial(prompt_kernel, group),
        out_shape=jax.ShapeDtypeStruct((steps, size, width + LANES), BF16),
        in_specs=[vmem] * 3,
        out_specs=vmem,
        compiler_params=params(12 if direct else 48),
        cost_estimate=cost(4 * size * steps * width * prefix_keys.shape[1], prefix_keys.size * 4),
        name="prompt",
    )
    answers = []
    for asked in received:
        answers.append(prompt(asked, keys, values))
    if direct:
        home = [answers[0]] + [swap(answers[i], "dp", i) for i in (1, 2, 3)]
    else:
        home = [all_to_all(answers[0])]

    attended = pl.pallas_call(
        functools.partial(merge_kernel, blocks),
        out_shape=jax.ShapeDtypeStruct((steps, count, width), BF16),
        in_specs=[vmem] * (blocks + 3),
        out_specs=vmem,
        compiler_params=params(8),
        cost_estimate=cost(2 * steps * owners * capacity * count * width, 2 << 20),
        name="merge",
    )(choice, *home, own_rows, own_logs)

    columns = out_weight.shape[1]
    if not direct:
        block_rows = lax.all_gather(attended, "dp", axis=1, tiled=True)
        product = jnp.dot(
            block_rows.reshape(-1, width), out_weight, preferred_element_type=F32
        ).reshape(steps, -1, columns)
        total = lax.psum_scatter(product, "kv", scatter_dimension=1, tiled=True)
        return total.astype(BF16).transpose(1, 0, 2)

    def move(values, pairs):
        return lax.ppermute(values, "dp", pairs)

    def across(values, inward):
        pairs = []
        for d in range(owners):
            for c in range(2):
                here, there = 2 * (d >> 1) + c, 2 * (1 - (d >> 1)) + c
                source, target = (there, here) if inward else (here, there)
                pairs.append((d * parts + source, d * parts + target))
        return lax.ppermute(values, ("dp", "kv"), pairs)

    chunk = columns // 4
    block = pl.BlockSpec((steps, count, width), lambda i: (0, 0, 0))
    narrow = pl.BlockSpec((steps, count, chunk), lambda i: (0, 0, i))

    def project(shifts, rows):
        return pl.pallas_call(
            functools.partial(project_kernel, shifts),
            grid=(columns // chunk,),
            out_shape=[
                jax.ShapeDtypeStruct((steps, count, columns), F32),
                jax.ShapeDtypeStruct((steps, count, columns), BF16),
            ],
            in_specs=[block] * len(rows) + [pl.BlockSpec((width, chunk), lambda i: (0, i))],
            out_specs=[narrow, narrow],
            scratch_shapes=[pltpu.VMEM((2, steps * count, width), BF16)],
            compiler_params=params(16),
            cost_estimate=cost(4 * steps * count * width * columns, out_weight.size * 2),
            name="project",
        )(*rows, out_weight)

    def add(keep, got):
        return pl.pallas_call(
            add_kernel,
            out_shape=[
                jax.ShapeDtypeStruct(keep.shape, F32),
                jax.ShapeDtypeStruct(keep.shape, BF16),
            ],
            in_specs=[vmem] * 2,
            out_specs=[vmem] * 2,
            compiler_params=params(4),
            cost_estimate=cost(keep.size, keep.size * 12),
            name="add",
        )(keep, got)

    beside = swap(attended, "dp", 1)
    middle = move(attended, [(1, 2), (2, 1)])
    far_in = move(attended, [(0, 2), (3, 1)])
    passed = move(middle, [(2, 3), (1, 0)])
    passed_far = move(far_in, [(2, 3), (1, 0)])
    near_keep, near_send = project((0, 1), [attended, beside])
    near_sum, near_send = add(near_keep, swap(near_send, "kv", 1))
    near_in = across(near_send, True)
    far_keep, far_send = project((2, 3), [far_in, passed, middle, passed_far])
    far_sum, far_send = add(far_keep, swap(far_send, "kv", 1))
    far_out = across(far_send, False)
    mine = lax.axis_index("kv") >> 1 == lax.axis_index("dp") >> 1
    total = jnp.where(mine, near_sum, far_sum) + near_in.astype(F32) + far_out.astype(F32)
    return total.astype(BF16).transpose(1, 0, 2)


def solution(mesh):
    placed = (
        P(("groups", "dp"), None, "kv"),
        P(("groups", "dp"), None),
        P(("groups", "dp")),
        P(("groups", "dp"), None, "kv"),
        P(("groups", "dp"), None, "kv"),
        P(("groups", "dp"), None, "kv"),
        P(("groups", "dp"), None, "kv"),
        P(("groups", "dp"), None, "kv"),
        P(("groups", "dp"), None, "kv"),
        P("kv", "dp"),
    )
    return jax.shard_map(
        local,
        mesh=mesh,
        in_specs=placed,
        out_specs=P(("groups", "kv"), None, "dp"),
        check_vma=False,
    )
```

```python
import functools
import math

import jax
import jax.numpy as jnp
from jax import lax
from jax.experimental import pallas as pl
from jax.experimental.pallas import tpu as pltpu
from jax.sharding import PartitionSpec as P


HD = 128
LANES = 128
F32 = jnp.float32
BF16 = jnp.bfloat16
HIDDEN = -1e30
MIB = 1 << 20
NT = (((1,), (1,)), ((), ()))


def params(mib):
    return pltpu.CompilerParams(vmem_limit_bytes=mib * MIB)


def cost(flops, nbytes, exps=0):
    return pl.CostEstimate(flops=flops, bytes_accessed=nbytes, transcendentals=exps)


def slots(routes_ref, count, capacity, base):
    names = [routes_ref[c] for c in range(count)]
    found = []
    for c in range(count):
        rank = jnp.int32(0)
        for earlier in range(c):
            rank = rank + (names[earlier] == names[c]).astype(jnp.int32)
        found.append((names[c] ^ base) * capacity + rank)
    return found


def spread(scalars, shape, dim):
    index = lax.broadcasted_iota(jnp.int32, shape, dim)
    out = jnp.full(shape, -1, jnp.int32)
    for c, value in enumerate(scalars):
        out = jnp.where(index == c, value, out)
    return out


def pack_kernel(capacity, relative, routes_ref, q_ref, held_ref, choice_ref, *refs):
    out_refs, (names, sems) = refs[:-2], refs[-2:]
    steps, count, _ = q_ref.shape
    name_copy = pltpu.make_async_copy(routes_ref, names, sems.at[0])
    q_copy = pltpu.make_async_copy(q_ref, held_ref, sems.at[1])
    name_copy.start()
    q_copy.start()
    base = lax.axis_index("dp") if relative else 0
    name_copy.wait()
    found = slots(names, count, capacity, base)
    shape = choice_ref.shape
    choice = spread(found, shape, 0) == lax.broadcasted_iota(jnp.int32, shape, 1)
    choice_ref[...] = choice.astype(BF16)
    shape = shape[::-1]
    placement = (spread(found, shape, 1) == lax.broadcasted_iota(jnp.int32, shape, 0)).astype(BF16)
    q_copy.wait()
    for s in range(steps):
        rows = jnp.dot(placement, held_ref[s], preferred_element_type=F32)
        at = 0
        for ref in out_refs:
            ref[s] = rows[at : at + ref.shape[1]].astype(BF16)
            at += ref.shape[1]


def suffix_kernel(
    group,
    q_ref,
    len_hbm,
    k_hbm,
    v_hbm,
    nk_hbm,
    nv_hbm,
    pk_hbm,
    pv_hbm,
    o_ref,
    l_ref,
    pk_ref,
    pv_ref,
    len_ref,
    k_ref,
    v_ref,
    nk_ref,
    nv_ref,
    qs,
    ss,
    ps,
    os,
    ls,
    sems,
):
    pairs = (
        (len_hbm, len_ref),
        (k_hbm, k_ref),
        (nk_hbm, nk_ref),
        (nv_hbm, nv_ref),
        (v_hbm, v_ref),
        (pk_hbm, pk_ref),
        (pv_hbm, pv_ref),
    )
    copies = [
        pltpu.make_async_copy(source, target, sems.at[i])
        for i, (source, target) in enumerate(pairs)
    ]
    for copy in copies:
        copy.start()
    steps, count, width = q_ref.shape
    heads = width // HD // group
    cached = k_ref.shape[1]
    each = steps * group
    rows = count * each
    scale = 1.0 / math.sqrt(HD)
    to_two = scale * math.log2(math.e)
    for h in range(heads):
        for s in range(steps):
            for g in range(group):
                piece = q_ref[s, :, pl.ds((h * group + g) * HD, HD)].astype(F32)
                qs[pl.ds(h * rows + s * group + g, count, stride=each), :] = piece
    row = lax.broadcasted_iota(jnp.int32, (rows, steps * count), 0).astype(F32)
    column = lax.broadcasted_iota(jnp.int32, (rows, steps * count), 1).astype(F32)
    row_cand = jnp.floor((row + 0.5) * (1.0 / each))
    row_step = jnp.floor((row - row_cand * each + 0.5) * (1.0 / group))
    key_step = jnp.floor((column + 0.5) * (1.0 / count))
    key_cand = column - key_step * count
    visible = (row_cand == key_cand) & (key_step <= row_step)
    position = lax.broadcasted_iota(jnp.int32, (each, cached), 1)
    for copy in copies[:4]:
        copy.wait()
    for h in range(heads):
        for c in range(count):
            qc = qs[pl.ds(h * rows + c * each, each), :].astype(BF16)
            kc = k_ref[c, :, pl.ds(h * HD, HD)]
            score = lax.dot_general(qc, kc, NT, preferred_element_type=F32)
            ss[pl.ds(c * each, each), :] = jnp.where(position < len_ref[c], score, HIDDEN)
        nk = jnp.concatenate([nk_ref[t, :, pl.ds(h * HD, HD)] for t in range(steps)], 0)
        nv = jnp.concatenate([nv_ref[t, :, pl.ds(h * HD, HD)] for t in range(steps)], 0)
        fresh = lax.dot_general(
            qs[pl.ds(h * rows, rows), :].astype(BF16), nk, NT, preferred_element_type=F32
        )
        fresh = jnp.where(visible, fresh, HIDDEN)
        score = ss[...]
        peak = jnp.maximum(
            jnp.max(score, -1, keepdims=True), jnp.max(fresh, -1, keepdims=True)
        )
        weight = jnp.exp2((score - peak) * to_two)
        fresh = jnp.exp2((fresh - peak) * to_two)
        total = jnp.sum(weight, -1, keepdims=True) + jnp.sum(fresh, -1, keepdims=True)
        ps[...] = weight.astype(BF16)
        if h == 0:
            copies[4].wait()
        os[...] = jnp.dot(fresh.astype(BF16), nv, preferred_element_type=F32)
        for c in range(count):
            vc = v_ref[c, :, pl.ds(h * HD, HD)]
            pc = ps[pl.ds(c * each, each), :]
            os[pl.ds(c * each, each), :] += jnp.dot(pc, vc, preferred_element_type=F32)
        os[...] = os[...] / total
        ls[...] = jnp.broadcast_to(peak * scale + jnp.log(total), ls.shape)
        for s in range(steps):
            for g in range(group):
                at = pl.ds(s * group + g, count, stride=each)
                lanes = pl.ds((h * group + g) * HD, HD)
                o_ref[s, :, lanes] = os[at, :]
                l_ref[s, :, lanes] = ls[at, :]
    for copy in copies[5:]:
        copy.wait()


def prompt_kernel(group, q_ref, k_ref, v_ref, out_ref):
    steps, size, width = q_ref.shape
    heads = width // HD // group
    all_heads = heads * group
    scale = 1.0 / math.sqrt(HD)
    to_two = scale * math.log2(math.e)
    lane = lax.broadcasted_iota(jnp.int32, (size, LANES), 1)
    place = lax.rem(lane, all_heads)
    logs = [jnp.zeros((size, LANES), F32) for _ in range(steps)]
    for h in range(heads):
        keys = k_ref[:, pl.ds(h * HD, HD)]
        values = v_ref[:, pl.ds(h * HD, HD)]
        q = jnp.concatenate(
            [
                q_ref[s, :, pl.ds((h * group + g) * HD, HD)]
                for s in range(steps)
                for g in range(group)
            ],
            0,
        )
        score = lax.dot_general(q, keys, NT, preferred_element_type=F32)
        peak = jnp.max(score, -1, keepdims=True)
        weight = jnp.exp2((score - peak) * to_two)
        total = jnp.sum(weight, -1, keepdims=True)
        out = jnp.dot(weight.astype(BF16), values, preferred_element_type=F32) / total
        log_total = peak * scale + jnp.log(total)
        for s in range(steps):
            for g in range(group):
                at = (s * group + g) * size
                lanes = pl.ds((h * group + g) * HD, HD)
                out_ref[s, :, lanes] = out[at : at + size].astype(BF16)
                logs[s] = jnp.where(place == h * group + g, log_total[at : at + size], logs[s])
    for s in range(steps):
        high = logs[s].astype(BF16).astype(F32)
        rest = logs[s] - high
        middle = rest.astype(BF16).astype(F32)
        low = rest - middle
        terms = jnp.where(lane < all_heads, high, jnp.where(lane < 2 * all_heads, middle, low))
        out_ref[s, :, pl.ds(width, LANES)] = terms.astype(BF16)


def merge_kernel(blocks, *refs):
    choice_ref, row_refs = refs[0], refs[1 : 1 + blocks]
    own_ref, log_ref, out_ref = refs[1 + blocks :]
    steps, count, width = own_ref.shape
    all_heads = width // HD
    choice = choice_ref[...]
    for s in range(steps):
        rows = jnp.concatenate([ref[s] for ref in row_refs], 0)
        rows = jnp.dot(choice, rows, preferred_element_type=F32)
        terms = rows[:, width:]
        logs = (
            terms[:, :all_heads]
            + terms[:, all_heads : 2 * all_heads]
            + terms[:, 2 * all_heads : 3 * all_heads]
        )
        for h in range(all_heads):
            lanes = slice(h * HD, (h + 1) * HD)
            first = jnp.broadcast_to(logs[:, h : h + 1], (count, HD))
            second = log_ref[s, :, lanes]
            peak = jnp.maximum(first, second)
            first = jnp.exp(first - peak)
            second = jnp.exp(second - peak)
            mixed = (first * rows[:, lanes] + second * own_ref[s, :, lanes]) / (first + second)
            out_ref[s, :, lanes] = mixed.astype(BF16)


def project_kernel(own_ref, g1_ref, g2_ref, g3_ref, w_ref, own_out, far_out, beside_out, held):
    steps, count, _ = own_ref.shape
    each = steps * count
    me, mine = lax.axis_index("dp"), lax.axis_index("kv")
    for shift, ref in enumerate((own_ref, g1_ref, g2_ref, g3_ref)):
        place = (me ^ shift) ^ mine
        for s in range(steps):
            held[place, pl.ds(s * count, count), :] = ref[s]
    rows = held[...].reshape(4 * each, held.shape[2])
    outs = (own_out, beside_out.at[0], far_out, beside_out.at[1])
    chunk = 512
    for at in range(0, w_ref.shape[1], chunk):
        lanes = pl.ds(at, chunk)
        product = jnp.dot(rows, w_ref[:, lanes], preferred_element_type=F32)
        for part, ref in enumerate(outs):
            for s in range(steps):
                row = part * each + s * count
                ref[s, :, lanes] = product[row : row + count].astype(ref.dtype)


def add_kernel(keep_ref, got_ref, send_ref):
    for s in range(keep_ref.shape[0]):
        send_ref[s] = (keep_ref[s] + got_ref[1, s].astype(F32)).astype(BF16)


def swap(values, axis, mask):
    pairs = [(i, i ^ mask) for i in range(lax.axis_size(axis))]
    return lax.ppermute(values, axis, pairs)


def local(
    queries,
    routes,
    suffix_lengths,
    prefix_keys,
    prefix_values,
    suffix_keys,
    suffix_values,
    new_keys,
    new_values,
    out_weight,
):
    owners, parts = lax.axis_size("dp"), lax.axis_size("kv")
    count, steps, width = queries.shape
    kv_width = prefix_keys.shape[2]
    heads = kv_width // HD
    group = width // kv_width
    capacity = max(2, 2 * count // owners)
    direct = owners == parts == 4 and capacity % 8 == 0
    blocks = owners if direct else 1
    size = capacity if direct else owners * capacity
    vmem, hbm = pl.BlockSpec(memory_space=pltpu.VMEM), pl.BlockSpec(memory_space=pltpu.HBM)
    far = lambda values: pltpu.with_memory_space_constraint(values, pltpu.HBM)
    names = routes.reshape(count)

    q, choice, *packed = pl.pallas_call(
        functools.partial(pack_kernel, capacity, direct),
        out_shape=[
            jax.ShapeDtypeStruct((steps, count, width), BF16),
            jax.ShapeDtypeStruct((count, owners * capacity), BF16),
        ]
        + [jax.ShapeDtypeStruct((steps, size, width), BF16)] * blocks,
        in_specs=[hbm, hbm],
        out_specs=[vmem] * (blocks + 2),
        scratch_shapes=[pltpu.SMEM((count,), jnp.int32), pltpu.SemaphoreType.DMA((2,))],
        compiler_params=params(8),
        cost_estimate=cost(2 * steps * owners * capacity * count * width, 1 << 20),
        name="pack",
    )(far(names), far(queries.transpose(1, 0, 2)))

    def all_to_all(values):
        values = values.reshape(steps, owners, capacity, -1)
        moved = lax.all_to_all(values, "dp", split_axis=1, concat_axis=1, tiled=True)
        return moved.reshape(steps, owners * capacity, -1)

    if direct:
        received = [packed[0]] + [swap(packed[i], "dp", i) for i in (1, 2, 3)]
    else:
        received = [all_to_all(packed[0])]

    rows = count * steps * group
    cached = suffix_keys.shape[1]
    new_shape = (steps, count, kv_width)
    own_rows, own_logs, keys, values = pl.pallas_call(
        functools.partial(suffix_kernel, group),
        out_shape=[jax.ShapeDtypeStruct((steps, count, width), F32)] * 2
        + [jax.ShapeDtypeStruct(prefix_keys.shape[1:], BF16)] * 2,
        in_specs=[vmem] + [hbm] * 7,
        out_specs=[vmem] * 4,
        scratch_shapes=[
            pltpu.SMEM((count,), jnp.int32),
            pltpu.VMEM(suffix_keys.shape, BF16),
            pltpu.VMEM(suffix_keys.shape, BF16),
            pltpu.VMEM(new_shape, BF16),
            pltpu.VMEM(new_shape, BF16),
            pltpu.VMEM((heads * rows, HD), F32),
            pltpu.VMEM((rows, cached), F32),
            pltpu.VMEM((rows, cached), BF16),
            pltpu.VMEM((rows, HD), F32),
            pltpu.VMEM((rows, LANES), F32),
            pltpu.SemaphoreType.DMA((7,)),
        ],
        compiler_params=params(16),
        cost_estimate=cost(3_000_000_000, suffix_keys.size * 4, rows * 512),
        name="suffix",
    )(
        q,
        far(suffix_lengths),
        far(suffix_keys),
        far(suffix_values),
        far(new_keys.transpose(1, 0, 2)),
        far(new_values.transpose(1, 0, 2)),
        far(prefix_keys[0]),
        far(prefix_values[0]),
    )

    prompt = pl.pallas_call(
        functools.partial(prompt_kernel, group),
        out_shape=jax.ShapeDtypeStruct((steps, size, width + LANES), BF16),
        in_specs=[vmem] * 3,
        out_specs=vmem,
        compiler_params=params(12 if direct else 48),
        cost_estimate=cost(4 * size * steps * width * prefix_keys.shape[1], prefix_keys.size * 4),
        name="prompt",
    )
    answers = []
    for asked in received:
        answers.append(prompt(asked, keys, values))
    if direct:
        home = [answers[0]] + [swap(answers[i], "dp", i) for i in (1, 2, 3)]
    else:
        home = [all_to_all(answers[0])]

    attended = pl.pallas_call(
        functools.partial(merge_kernel, blocks),
        out_shape=jax.ShapeDtypeStruct((steps, count, width), BF16),
        in_specs=[vmem] * (blocks + 3),
        out_specs=vmem,
        compiler_params=params(8),
        cost_estimate=cost(2 * steps * owners * capacity * count * width, 2 << 20),
        name="merge",
    )(choice, *home, own_rows, own_logs)

    columns = out_weight.shape[1]
    if not direct:
        block_rows = lax.all_gather(attended, "dp", axis=1, tiled=True)
        product = jnp.dot(
            block_rows.reshape(-1, width), out_weight, preferred_element_type=F32
        ).reshape(steps, -1, columns)
        total = lax.psum_scatter(product, "kv", scatter_dimension=1, tiled=True)
        return total.astype(BF16).transpose(1, 0, 2)

    by_two = swap(attended, "dp", 2)
    by_one = swap(attended, "dp", 1)
    by_three = swap(attended, "dp", 3)
    piece = (steps, count, columns)
    own_sum, far_sum, beside = pl.pallas_call(
        project_kernel,
        out_shape=[
            jax.ShapeDtypeStruct(piece, F32),
            jax.ShapeDtypeStruct(piece, F32),
            jax.ShapeDtypeStruct((2, *piece), BF16),
        ],
        in_specs=[vmem] * 5,
        out_specs=[vmem] * 3,
        scratch_shapes=[pltpu.VMEM((owners, steps * count, width), BF16)],
        compiler_params=params(8),
        cost_estimate=cost(2 * owners * steps * count * width * columns, out_weight.size * 2),
        name="project",
    )(attended, by_one, by_two, by_three, out_weight)
    got = swap(beside, "kv", 1)
    sent = pl.pallas_call(
        add_kernel,
        out_shape=jax.ShapeDtypeStruct(piece, BF16),
        in_specs=[vmem] * 2,
        out_specs=vmem,
        compiler_params=params(4),
        cost_estimate=cost(far_sum.size, far_sum.size * 12),
        name="add",
    )(far_sum, got)
    came = swap(sent, "kv", 2)
    total = own_sum + got[0].astype(F32) + came.astype(F32)
    return total.astype(BF16).transpose(1, 0, 2)


def solution(mesh):
    placed = (
        P(("groups", "dp"), None, "kv"),
        P(("groups", "dp"), None),
        P(("groups", "dp")),
        P(("groups", "dp"), None, "kv"),
        P(("groups", "dp"), None, "kv"),
        P(("groups", "dp"), None, "kv"),
        P(("groups", "dp"), None, "kv"),
        P(("groups", "dp"), None, "kv"),
        P(("groups", "dp"), None, "kv"),
        P("kv", "dp"),
    )
    return jax.shard_map(
        local,
        mesh=mesh,
        in_specs=placed,
        out_specs=P(("groups", "kv"), None, "dp"),
        check_vma=False,
    )
```

```python
import functools
import math

import jax
import jax.numpy as jnp
from jax import lax
from jax.experimental import pallas as pl
from jax.experimental.pallas import tpu as pltpu
from jax.sharding import PartitionSpec as P


HD = 128
LANES = 128
F32 = jnp.float32
BF16 = jnp.bfloat16
HIDDEN = -1e30
MIB = 1 << 20
PIECES = 4
HALVES = 2
NT = (((1,), (1,)), ((), ()))


def params(mib):
    return pltpu.CompilerParams(vmem_limit_bytes=mib * MIB)


def cost(flops, nbytes, exps=0):
    return pl.CostEstimate(flops=flops, bytes_accessed=nbytes, transcendentals=exps)


def slots(routes_ref, count, capacity, base):
    names = [routes_ref[c] for c in range(count)]
    found = []
    for c in range(count):
        rank = jnp.int32(0)
        for earlier in range(c):
            rank = rank + (names[earlier] == names[c]).astype(jnp.int32)
        found.append((names[c] ^ base) * capacity + rank)
    return found


def spread(scalars, shape, dim):
    index = lax.broadcasted_iota(jnp.int32, shape, dim)
    out = jnp.full(shape, -1, jnp.int32)
    for c, value in enumerate(scalars):
        out = jnp.where(index == c, value, out)
    return out


def pack_kernel(capacity, relative, routes_ref, q_ref, held_ref, choice_ref, *refs):
    out_refs, (names, sems) = refs[:-2], refs[-2:]
    steps, count, _ = q_ref.shape
    name_copy = pltpu.make_async_copy(routes_ref, names, sems.at[0])
    q_copy = pltpu.make_async_copy(q_ref, held_ref, sems.at[1])
    name_copy.start()
    q_copy.start()
    base = lax.axis_index("dp") if relative else 0
    name_copy.wait()
    found = slots(names, count, capacity, base)
    shape = choice_ref.shape
    choice = spread(found, shape, 0) == lax.broadcasted_iota(jnp.int32, shape, 1)
    choice_ref[...] = choice.astype(BF16)
    shape = shape[::-1]
    placement = (spread(found, shape, 1) == lax.broadcasted_iota(jnp.int32, shape, 0)).astype(BF16)
    q_copy.wait()
    for s in range(steps):
        rows = jnp.dot(placement, held_ref[s], preferred_element_type=F32)
        at = 0
        for ref in out_refs:
            ref[s] = rows[at : at + ref.shape[1]].astype(BF16)
            at += ref.shape[1]


def suffix_kernel(
    group,
    q_ref,
    len_hbm,
    k_hbm,
    v_hbm,
    nk_hbm,
    nv_hbm,
    o_ref,
    l_ref,
    len_ref,
    k_ref,
    v_ref,
    nk_ref,
    nv_ref,
    qs,
    ss,
    ps,
    os,
    ls,
    sems,
):
    pairs = (
        (len_hbm, len_ref),
        (k_hbm, k_ref),
        (nk_hbm, nk_ref),
        (nv_hbm, nv_ref),
        (v_hbm, v_ref),
    )
    copies = [
        pltpu.make_async_copy(source, target, sems.at[i])
        for i, (source, target) in enumerate(pairs)
    ]
    for copy in copies:
        copy.start()
    steps, count, width = q_ref.shape
    heads = width // HD // group
    cached = k_ref.shape[1]
    each = steps * group
    rows = count * each
    scale = 1.0 / math.sqrt(HD)
    to_two = scale * math.log2(math.e)
    for h in range(heads):
        for s in range(steps):
            for g in range(group):
                piece = q_ref[s, :, pl.ds((h * group + g) * HD, HD)].astype(F32)
                qs[pl.ds(h * rows + s * group + g, count, stride=each), :] = piece
    row = lax.broadcasted_iota(jnp.int32, (rows, steps * count), 0).astype(F32)
    column = lax.broadcasted_iota(jnp.int32, (rows, steps * count), 1).astype(F32)
    row_cand = jnp.floor((row + 0.5) * (1.0 / each))
    row_step = jnp.floor((row - row_cand * each + 0.5) * (1.0 / group))
    key_step = jnp.floor((column + 0.5) * (1.0 / count))
    key_cand = column - key_step * count
    visible = (row_cand == key_cand) & (key_step <= row_step)
    position = lax.broadcasted_iota(jnp.int32, (each, cached), 1)
    for copy in copies[:4]:
        copy.wait()
    for h in range(heads):
        for c in range(count):
            qc = qs[pl.ds(h * rows + c * each, each), :].astype(BF16)
            kc = k_ref[c, :, pl.ds(h * HD, HD)]
            score = lax.dot_general(qc, kc, NT, preferred_element_type=F32)
            ss[pl.ds(c * each, each), :] = jnp.where(position < len_ref[c], score, HIDDEN)
        nk = jnp.concatenate([nk_ref[t, :, pl.ds(h * HD, HD)] for t in range(steps)], 0)
        nv = jnp.concatenate([nv_ref[t, :, pl.ds(h * HD, HD)] for t in range(steps)], 0)
        fresh = lax.dot_general(
            qs[pl.ds(h * rows, rows), :].astype(BF16), nk, NT, preferred_element_type=F32
        )
        fresh = jnp.where(visible, fresh, HIDDEN)
        score = ss[...]
        peak = jnp.maximum(
            jnp.max(score, -1, keepdims=True), jnp.max(fresh, -1, keepdims=True)
        )
        weight = jnp.exp2((score - peak) * to_two)
        fresh = jnp.exp2((fresh - peak) * to_two)
        total = jnp.sum(weight, -1, keepdims=True) + jnp.sum(fresh, -1, keepdims=True)
        ps[...] = weight.astype(BF16)
        if h == 0:
            copies[4].wait()
        os[...] = jnp.dot(fresh.astype(BF16), nv, preferred_element_type=F32)
        for c in range(count):
            vc = v_ref[c, :, pl.ds(h * HD, HD)]
            pc = ps[pl.ds(c * each, each), :]
            os[pl.ds(c * each, each), :] += jnp.dot(pc, vc, preferred_element_type=F32)
        os[...] = os[...] / total
        ls[...] = jnp.broadcast_to(peak * scale + jnp.log(total), ls.shape)
        for s in range(steps):
            for g in range(group):
                at = pl.ds(s * group + g, count, stride=each)
                lanes = pl.ds((h * group + g) * HD, HD)
                o_ref[s, :, lanes] = os[at, :]
                l_ref[s, :, lanes] = ls[at, :]


def load_kernel(k_hbm, v_hbm, k_ref, v_ref, sems):
    copies = []
    for source, target in ((k_hbm, k_ref), (v_hbm, v_ref)):
        part = source.shape[0] // PIECES
        for at in range(0, source.shape[0], part):
            pair = source.at[pl.ds(at, part)], target.at[pl.ds(at, part)]
            copies.append(pltpu.make_async_copy(*pair, sems.at[len(copies)]))
    for copy in copies:
        copy.start()
    for copy in copies:
        copy.wait()


def prompt_kernel(group, q_ref, k_ref, v_ref, out_ref):
    steps, size, width = q_ref.shape
    heads = width // HD // group
    all_heads = heads * group
    scale = 1.0 / math.sqrt(HD)
    to_two = scale * math.log2(math.e)
    lane = lax.broadcasted_iota(jnp.int32, (size, LANES), 1)
    place = lax.rem(lane, all_heads)
    logs = [jnp.zeros((size, LANES), F32) for _ in range(steps)]
    for h in range(heads):
        keys = k_ref[:, pl.ds(h * HD, HD)]
        values = v_ref[:, pl.ds(h * HD, HD)]
        q = jnp.concatenate(
            [
                q_ref[s, :, pl.ds((h * group + g) * HD, HD)]
                for s in range(steps)
                for g in range(group)
            ],
            0,
        )
        score = lax.dot_general(q, keys, NT, preferred_element_type=F32)
        peak = jnp.max(score, -1, keepdims=True)
        weight = jnp.exp2((score - peak) * to_two)
        total = jnp.sum(weight, -1, keepdims=True)
        out = jnp.dot(weight.astype(BF16), values, preferred_element_type=F32) / total
        log_total = peak * scale + jnp.log(total)
        for s in range(steps):
            for g in range(group):
                at = (s * group + g) * size
                lanes = pl.ds((h * group + g) * HD, HD)
                out_ref[s, :, lanes] = out[at : at + size].astype(BF16)
                logs[s] = jnp.where(place == h * group + g, log_total[at : at + size], logs[s])
    for s in range(steps):
        high = logs[s].astype(BF16).astype(F32)
        rest = logs[s] - high
        middle = rest.astype(BF16).astype(F32)
        low = rest - middle
        terms = jnp.where(lane < all_heads, high, jnp.where(lane < 2 * all_heads, middle, low))
        out_ref[s, :, pl.ds(width, LANES)] = terms.astype(BF16)


def merge_kernel(blocks, *refs):
    choice_ref, row_refs = refs[0], refs[1 : 1 + blocks]
    own_ref, log_ref, out_ref = refs[1 + blocks :]
    steps, count, width = own_ref.shape
    all_heads = width // HD
    choice = choice_ref[...]
    for s in range(steps):
        rows = jnp.concatenate([ref[s] for ref in row_refs], 0)
        rows = jnp.dot(choice, rows, preferred_element_type=F32)
        terms = rows[:, width:]
        logs = (
            terms[:, :all_heads]
            + terms[:, all_heads : 2 * all_heads]
            + terms[:, 2 * all_heads : 3 * all_heads]
        )
        for h in range(all_heads):
            lanes = slice(h * HD, (h + 1) * HD)
            first = jnp.broadcast_to(logs[:, h : h + 1], (count, HD))
            second = log_ref[s, :, lanes]
            peak = jnp.maximum(first, second)
            first = jnp.exp(first - peak)
            second = jnp.exp(second - peak)
            mixed = (first * rows[:, lanes] + second * own_ref[s, :, lanes]) / (first + second)
            out_ref[s, :, lanes] = mixed.astype(BF16)


def project_kernel(first, own_ref, g1_ref, g2_ref, g3_ref, w_ref, own_out, far_out, beside_out, held):
    steps, count, _ = own_ref.shape
    each = steps * count
    me, mine = lax.axis_index("dp"), lax.axis_index("kv")
    for shift, ref in enumerate((own_ref, g1_ref, g2_ref, g3_ref)):
        place = (me ^ shift) ^ mine
        for s in range(steps):
            held[place, pl.ds(s * count, count), :] = ref[s]
    rows = held[...].reshape(4 * each, held.shape[2])
    outs = (own_out, beside_out.at[0], far_out, beside_out.at[1])
    chunk = 512
    for at in range(0, own_out.shape[2], chunk):
        lanes = pl.ds(at, chunk)
        product = jnp.dot(rows, w_ref[:, pl.ds(first + at, chunk)], preferred_element_type=F32)
        for part, ref in enumerate(outs):
            for s in range(steps):
                row = part * each + s * count
                ref[s, :, lanes] = product[row : row + count].astype(ref.dtype)


def add_kernel(keep_ref, got_ref, send_ref):
    for s in range(keep_ref.shape[0]):
        send_ref[s] = (keep_ref[s] + got_ref[1, s].astype(F32)).astype(BF16)


def swap(values, axis, mask):
    pairs = [(i, i ^ mask) for i in range(lax.axis_size(axis))]
    return lax.ppermute(values, axis, pairs)


def local(
    queries,
    routes,
    suffix_lengths,
    prefix_keys,
    prefix_values,
    suffix_keys,
    suffix_values,
    new_keys,
    new_values,
    out_weight,
):
    owners, parts = lax.axis_size("dp"), lax.axis_size("kv")
    count, steps, width = queries.shape
    kv_width = prefix_keys.shape[2]
    heads = kv_width // HD
    group = width // kv_width
    capacity = max(2, 2 * count // owners)
    direct = owners == parts == 4 and capacity % 8 == 0
    blocks = owners if direct else 1
    size = capacity if direct else owners * capacity
    vmem, hbm = pl.BlockSpec(memory_space=pltpu.VMEM), pl.BlockSpec(memory_space=pltpu.HBM)
    far = lambda values: pltpu.with_memory_space_constraint(values, pltpu.HBM)
    names = routes.reshape(count)

    q, choice, *packed = pl.pallas_call(
        functools.partial(pack_kernel, capacity, direct),
        out_shape=[
            jax.ShapeDtypeStruct((steps, count, width), BF16),
            jax.ShapeDtypeStruct((count, owners * capacity), BF16),
        ]
        + [jax.ShapeDtypeStruct((steps, size, width), BF16)] * blocks,
        in_specs=[hbm, hbm],
        out_specs=[vmem] * (blocks + 2),
        scratch_shapes=[pltpu.SMEM((count,), jnp.int32), pltpu.SemaphoreType.DMA((2,))],
        compiler_params=params(8),
        cost_estimate=cost(2 * steps * owners * capacity * count * width, 1 << 20),
        name="pack",
    )(far(names), far(queries.transpose(1, 0, 2)))

    def all_to_all(values):
        values = values.reshape(steps, owners, capacity, -1)
        moved = lax.all_to_all(values, "dp", split_axis=1, concat_axis=1, tiled=True)
        return moved.reshape(steps, owners * capacity, -1)

    if direct:
        received = [packed[0]] + [swap(packed[i], "dp", i) for i in (1, 2, 3)]
    else:
        received = [all_to_all(packed[0])]

    rows = count * steps * group
    cached = suffix_keys.shape[1]
    new_shape = (steps, count, kv_width)
    keys, values = pl.pallas_call(
        load_kernel,
        out_shape=[jax.ShapeDtypeStruct(prefix_keys.shape[1:], BF16)] * 2,
        in_specs=[hbm] * 2,
        out_specs=[vmem] * 2,
        scratch_shapes=[pltpu.SemaphoreType.DMA((2 * PIECES,))],
        compiler_params=params(4),
        cost_estimate=cost(500_000_000, prefix_keys.size * 4),
        name="load",
    )(far(prefix_keys[0]), far(prefix_values[0]))
    own_rows, own_logs = pl.pallas_call(
        functools.partial(suffix_kernel, group),
        out_shape=[jax.ShapeDtypeStruct((steps, count, width), F32)] * 2,
        in_specs=[vmem] + [hbm] * 5,
        out_specs=[vmem] * 2,
        scratch_shapes=[
            pltpu.SMEM((count,), jnp.int32),
            pltpu.VMEM(suffix_keys.shape, BF16),
            pltpu.VMEM(suffix_keys.shape, BF16),
            pltpu.VMEM(new_shape, BF16),
            pltpu.VMEM(new_shape, BF16),
            pltpu.VMEM((heads * rows, HD), F32),
            pltpu.VMEM((rows, cached), F32),
            pltpu.VMEM((rows, cached), BF16),
            pltpu.VMEM((rows, HD), F32),
            pltpu.VMEM((rows, LANES), F32),
            pltpu.SemaphoreType.DMA((5,)),
        ],
        compiler_params=params(16),
        cost_estimate=cost(3_000_000_000, suffix_keys.size * 4, rows * 512),
        name="suffix",
    )(
        q,
        far(suffix_lengths),
        far(suffix_keys),
        far(suffix_values),
        far(new_keys.transpose(1, 0, 2)),
        far(new_values.transpose(1, 0, 2)),
    )

    prompt = pl.pallas_call(
        functools.partial(prompt_kernel, group),
        out_shape=jax.ShapeDtypeStruct((steps, size, width + LANES), BF16),
        in_specs=[vmem] * 3,
        out_specs=vmem,
        compiler_params=params(12 if direct else 48),
        cost_estimate=cost(4 * size * steps * width * prefix_keys.shape[1], prefix_keys.size * 4),
        name="prompt",
    )
    answers = []
    for asked in received:
        answers.append(prompt(asked, keys, values))
    if direct:
        home = [answers[0]] + [swap(answers[i], "dp", i) for i in (1, 2, 3)]
    else:
        home = [all_to_all(answers[0])]

    attended = pl.pallas_call(
        functools.partial(merge_kernel, blocks),
        out_shape=jax.ShapeDtypeStruct((steps, count, width), BF16),
        in_specs=[vmem] * (blocks + 3),
        out_specs=vmem,
        compiler_params=params(8),
        cost_estimate=cost(2 * steps * owners * capacity * count * width, 2 << 20),
        name="merge",
    )(choice, *home, own_rows, own_logs)

    columns = out_weight.shape[1]
    if not direct:
        block_rows = lax.all_gather(attended, "dp", axis=1, tiled=True)
        product = jnp.dot(
            block_rows.reshape(-1, width), out_weight, preferred_element_type=F32
        ).reshape(steps, -1, columns)
        total = lax.psum_scatter(product, "kv", scatter_dimension=1, tiled=True)
        return total.astype(BF16).transpose(1, 0, 2)

    by_two = swap(attended, "dp", 2)
    by_one = swap(attended, "dp", 1)
    by_three = swap(by_two, "dp", 1)
    half = columns // HALVES
    piece = (steps, count, half)

    def reduced(part):
        own_sum, far_sum, beside = pl.pallas_call(
            functools.partial(project_kernel, part * half),
            out_shape=[
                jax.ShapeDtypeStruct(piece, F32),
                jax.ShapeDtypeStruct(piece, F32),
                jax.ShapeDtypeStruct((2, *piece), BF16),
            ],
            in_specs=[vmem] * 5,
            out_specs=[vmem] * 3,
            scratch_shapes=[pltpu.VMEM((owners, steps * count, width), BF16)],
            compiler_params=params(8),
            cost_estimate=cost(2 * owners * steps * count * width * half, width * half * 2),
        )(attended, by_one, by_two, by_three, out_weight)
        got = swap(beside, "kv", 1)
        sent = pl.pallas_call(
            add_kernel,
            out_shape=jax.ShapeDtypeStruct(piece, BF16),
            in_specs=[vmem] * 2,
            out_specs=vmem,
            compiler_params=params(4),
            cost_estimate=cost(far_sum.size, far_sum.size * 12),
        )(far_sum, got)
        came = swap(sent, "kv", 2)
        return own_sum, got, came

    sums = [reduced(part) for part in range(HALVES)]

    def total_kernel(*refs):
        *in_refs, out_ref = refs
        for part in range(HALVES):
            own_ref, got_ref, came_ref = in_refs[3 * part : 3 * part + 3]
            for s in range(steps):
                total = own_ref[s] + got_ref[0, s].astype(F32) + came_ref[s].astype(F32)
                out_ref[s, :, pl.ds(part * half, half)] = total.astype(BF16)

    total = pl.pallas_call(
        total_kernel,
        out_shape=jax.ShapeDtypeStruct((steps, count, columns), BF16),
        in_specs=[vmem] * (3 * HALVES),
        out_specs=vmem,
        compiler_params=params(8),
        cost_estimate=cost(columns * count * steps, columns * count * steps * 12),
        name="total",
    )(*[value for part in sums for value in part])
    return total.transpose(1, 0, 2)


def solution(mesh):
    placed = (
        P(("groups", "dp"), None, "kv"),
        P(("groups", "dp"), None),
        P(("groups", "dp")),
        P(("groups", "dp"), None, "kv"),
        P(("groups", "dp"), None, "kv"),
        P(("groups", "dp"), None, "kv"),
        P(("groups", "dp"), None, "kv"),
        P(("groups", "dp"), None, "kv"),
        P(("groups", "dp"), None, "kv"),
        P("kv", "dp"),
    )
    return jax.shard_map(
        local,
        mesh=mesh,
        in_specs=placed,
        out_specs=P(("groups", "kv"), None, "dp"),
        check_vma=False,
    )
```

```python
import functools
import math

import jax
import jax.numpy as jnp
from jax import lax
from jax.experimental import pallas as pl
from jax.experimental.pallas import tpu as pltpu
from jax.sharding import PartitionSpec as P


HD = 128
LANES = 128
F32 = jnp.float32
BF16 = jnp.bfloat16
HIDDEN = -1e30
MIB = 1 << 20
PIECES = 4
NT = (((1,), (1,)), ((), ()))


def params(mib):
    return pltpu.CompilerParams(vmem_limit_bytes=mib * MIB)


def cost(flops, nbytes, exps=0):
    return pl.CostEstimate(flops=flops, bytes_accessed=nbytes, transcendentals=exps)


def slots(routes_ref, count, capacity, base):
    names = [routes_ref[c] for c in range(count)]
    found = []
    for c in range(count):
        rank = jnp.int32(0)
        for earlier in range(c):
            rank = rank + (names[earlier] == names[c]).astype(jnp.int32)
        found.append((names[c] ^ base) * capacity + rank)
    return found


def spread(scalars, shape, dim):
    index = lax.broadcasted_iota(jnp.int32, shape, dim)
    out = jnp.full(shape, -1, jnp.int32)
    for c, value in enumerate(scalars):
        out = jnp.where(index == c, value, out)
    return out


def pack_kernel(capacity, relative, routes_ref, q_ref, held_ref, choice_ref, *refs):
    out_refs, (names, sems) = refs[:-2], refs[-2:]
    steps, count, _ = q_ref.shape
    name_copy = pltpu.make_async_copy(routes_ref, names, sems.at[0])
    q_copy = pltpu.make_async_copy(q_ref, held_ref, sems.at[1])
    name_copy.start()
    q_copy.start()
    base = lax.axis_index("dp") if relative else 0
    name_copy.wait()
    found = slots(names, count, capacity, base)
    shape = choice_ref.shape
    choice = spread(found, shape, 0) == lax.broadcasted_iota(jnp.int32, shape, 1)
    choice_ref[...] = choice.astype(BF16)
    shape = shape[::-1]
    placement = (spread(found, shape, 1) == lax.broadcasted_iota(jnp.int32, shape, 0)).astype(BF16)
    q_copy.wait()
    for s in range(steps):
        rows = jnp.dot(placement, held_ref[s], preferred_element_type=F32)
        at = 0
        for ref in out_refs:
            ref[s] = rows[at : at + ref.shape[1]].astype(BF16)
            at += ref.shape[1]


def suffix_kernel(
    group,
    q_ref,
    len_hbm,
    k_hbm,
    v_hbm,
    nk_hbm,
    nv_hbm,
    o_ref,
    l_ref,
    len_ref,
    k_ref,
    v_ref,
    nk_ref,
    nv_ref,
    qs,
    ss,
    ps,
    os,
    ls,
    sems,
):
    pairs = (
        (len_hbm, len_ref),
        (k_hbm, k_ref),
        (nk_hbm, nk_ref),
        (nv_hbm, nv_ref),
        (v_hbm, v_ref),
    )
    copies = [
        pltpu.make_async_copy(source, target, sems.at[i])
        for i, (source, target) in enumerate(pairs)
    ]
    for copy in copies:
        copy.start()
    steps, count, width = q_ref.shape
    heads = width // HD // group
    cached = k_ref.shape[1]
    each = steps * group
    rows = count * each
    scale = 1.0 / math.sqrt(HD)
    to_two = scale * math.log2(math.e)
    for h in range(heads):
        for s in range(steps):
            for g in range(group):
                piece = q_ref[s, :, pl.ds((h * group + g) * HD, HD)].astype(F32)
                qs[pl.ds(h * rows + s * group + g, count, stride=each), :] = piece
    row = lax.broadcasted_iota(jnp.int32, (rows, steps * count), 0).astype(F32)
    column = lax.broadcasted_iota(jnp.int32, (rows, steps * count), 1).astype(F32)
    row_cand = jnp.floor((row + 0.5) * (1.0 / each))
    row_step = jnp.floor((row - row_cand * each + 0.5) * (1.0 / group))
    key_step = jnp.floor((column + 0.5) * (1.0 / count))
    key_cand = column - key_step * count
    visible = (row_cand == key_cand) & (key_step <= row_step)
    position = lax.broadcasted_iota(jnp.int32, (each, cached), 1)
    for copy in copies[:4]:
        copy.wait()
    for h in range(heads):
        for c in range(count):
            qc = qs[pl.ds(h * rows + c * each, each), :].astype(BF16)
            kc = k_ref[c, :, pl.ds(h * HD, HD)]
            score = lax.dot_general(qc, kc, NT, preferred_element_type=F32)
            ss[pl.ds(c * each, each), :] = jnp.where(position < len_ref[c], score, HIDDEN)
        nk = jnp.concatenate([nk_ref[t, :, pl.ds(h * HD, HD)] for t in range(steps)], 0)
        nv = jnp.concatenate([nv_ref[t, :, pl.ds(h * HD, HD)] for t in range(steps)], 0)
        fresh = lax.dot_general(
            qs[pl.ds(h * rows, rows), :].astype(BF16), nk, NT, preferred_element_type=F32
        )
        fresh = jnp.where(visible, fresh, HIDDEN)
        score = ss[...]
        peak = jnp.maximum(
            jnp.max(score, -1, keepdims=True), jnp.max(fresh, -1, keepdims=True)
        )
        weight = jnp.exp2((score - peak) * to_two)
        fresh = jnp.exp2((fresh - peak) * to_two)
        total = jnp.sum(weight, -1, keepdims=True) + jnp.sum(fresh, -1, keepdims=True)
        ps[...] = weight.astype(BF16)
        if h == 0:
            copies[4].wait()
        os[...] = jnp.dot(fresh.astype(BF16), nv, preferred_element_type=F32)
        for c in range(count):
            vc = v_ref[c, :, pl.ds(h * HD, HD)]
            pc = ps[pl.ds(c * each, each), :]
            os[pl.ds(c * each, each), :] += jnp.dot(pc, vc, preferred_element_type=F32)
        os[...] = os[...] / total
        ls[...] = jnp.broadcast_to(peak * scale + jnp.log(total), ls.shape)
        for s in range(steps):
            for g in range(group):
                at = pl.ds(s * group + g, count, stride=each)
                lanes = pl.ds((h * group + g) * HD, HD)
                o_ref[s, :, lanes] = os[at, :]
                l_ref[s, :, lanes] = ls[at, :]


def load_kernel(k_hbm, v_hbm, k_ref, v_ref, sems):
    copies = []
    for source, target in ((k_hbm, k_ref), (v_hbm, v_ref)):
        part = source.shape[0] // PIECES
        for at in range(0, source.shape[0], part):
            pair = source.at[pl.ds(at, part)], target.at[pl.ds(at, part)]
            copies.append(pltpu.make_async_copy(*pair, sems.at[len(copies)]))
    for copy in copies:
        copy.start()
    for copy in copies:
        copy.wait()


def prompt_kernel(group, q_ref, k_ref, v_ref, out_ref):
    steps, size, width = q_ref.shape
    heads = width // HD // group
    all_heads = heads * group
    scale = 1.0 / math.sqrt(HD)
    to_two = scale * math.log2(math.e)
    lane = lax.broadcasted_iota(jnp.int32, (size, LANES), 1)
    place = lax.rem(lane, all_heads)
    logs = [jnp.zeros((size, LANES), F32) for _ in range(steps)]
    scores = []
    for h in range(heads):
        q = jnp.concatenate(
            [
                q_ref[s, :, pl.ds((h * group + g) * HD, HD)]
                for s in range(steps)
                for g in range(group)
            ],
            0,
        )
        keys = k_ref[:, pl.ds(h * HD, HD)]
        scores.append(lax.dot_general(q, keys, NT, preferred_element_type=F32))
    for h in range(heads):
        values = v_ref[:, pl.ds(h * HD, HD)]
        score = scores[h]
        peak = jnp.max(score, -1, keepdims=True)
        weight = jnp.exp2((score - peak) * to_two)
        total = jnp.sum(weight, -1, keepdims=True)
        out = jnp.dot(weight.astype(BF16), values, preferred_element_type=F32) / total
        log_total = peak * scale + jnp.log(total)
        for s in range(steps):
            for g in range(group):
                at = (s * group + g) * size
                lanes = pl.ds((h * group + g) * HD, HD)
                out_ref[s, :, lanes] = out[at : at + size].astype(BF16)
                logs[s] = jnp.where(place == h * group + g, log_total[at : at + size], logs[s])
    for s in range(steps):
        high = logs[s].astype(BF16).astype(F32)
        rest = logs[s] - high
        middle = rest.astype(BF16).astype(F32)
        low = rest - middle
        terms = jnp.where(lane < all_heads, high, jnp.where(lane < 2 * all_heads, middle, low))
        out_ref[s, :, pl.ds(width, LANES)] = terms.astype(BF16)


def merge_kernel(blocks, *refs):
    choice_ref, row_refs = refs[0], refs[1 : 1 + blocks]
    own_ref, log_ref, out_ref = refs[1 + blocks :]
    steps, count, width = own_ref.shape
    all_heads = width // HD
    choice = choice_ref[...]
    for s in range(steps):
        rows = jnp.concatenate([ref[s] for ref in row_refs], 0)
        rows = jnp.dot(choice, rows, preferred_element_type=F32)
        terms = rows[:, width:]
        logs = (
            terms[:, :all_heads]
            + terms[:, all_heads : 2 * all_heads]
            + terms[:, 2 * all_heads : 3 * all_heads]
        )
        for h in range(all_heads):
            lanes = slice(h * HD, (h + 1) * HD)
            first = jnp.broadcast_to(logs[:, h : h + 1], (count, HD))
            second = log_ref[s, :, lanes]
            peak = jnp.maximum(first, second)
            first = jnp.exp(first - peak)
            second = jnp.exp(second - peak)
            mixed = (first * rows[:, lanes] + second * own_ref[s, :, lanes]) / (first + second)
            out_ref[s, :, lanes] = mixed.astype(BF16)


CHUNK = 512


def early_kernel(own_ref, g1_ref, g2_ref, w_ref, own_out, far_out, beside_out, held):
    steps, count, _ = own_ref.shape
    each = steps * count
    me, mine = lax.axis_index("dp"), lax.axis_index("kv")
    for shift, ref in enumerate((own_ref, g1_ref, g2_ref)):
        place = (me ^ shift) ^ mine
        for s in range(steps):
            held[place, pl.ds(s * count, count), :] = ref[s]
    held[(me ^ 3) ^ mine, :, :] = jnp.zeros(held.shape[1:], BF16)
    rows = held[...].reshape(4 * each, held.shape[2])
    outs = (own_out, beside_out.at[0], far_out, beside_out.at[1])
    for at in range(0, w_ref.shape[1], CHUNK):
        lanes = pl.ds(at, CHUNK)
        product = jnp.dot(rows, w_ref[:, lanes], preferred_element_type=F32)
        for part, ref in enumerate(outs):
            for s in range(steps):
                row = part * each + s * count
                ref[s, :, lanes] = product[row : row + count].astype(ref.dtype)


def late_kernel(rows_ref, w_ref, keep_out, send_out, held):
    steps, count, half = keep_out.shape
    core = lax.axis_index("kv") & 1
    for s in range(steps):
        held[pl.ds(s * count, count), :] = rows_ref[s]
    for which, ref in ((1, send_out), (0, keep_out)):
        for at in range(0, half, CHUNK):
            first = pl.multiple_of((core ^ which) * half + at, CHUNK)
            product = jnp.dot(held[...], w_ref[:, pl.ds(first, CHUNK)], preferred_element_type=F32)
            for s in range(steps):
                ref[s, :, pl.ds(at, CHUNK)] = product[s * count : (s + 1) * count].astype(ref.dtype)


def add_kernel(keep_ref, got_ref, send_ref):
    for s in range(keep_ref.shape[0]):
        send_ref[s] = (keep_ref[s] + got_ref[1, s].astype(F32)).astype(BF16)


def late_add_kernel(keep_ref, got_ref, sum_ref, send_ref):
    for s in range(keep_ref.shape[0]):
        total = keep_ref[s] + got_ref[s].astype(F32)
        sum_ref[s] = total
        send_ref[s] = total.astype(BF16)


def total_kernel(own_ref, got_ref, came_ref, half_ref, other_ref, out_ref):
    steps, _, half = half_ref.shape
    kv = lax.axis_index("kv")
    here = kv == (lax.axis_index("dp") ^ 3)
    for which, ref in ((0, half_ref), (1, other_ref)):
        lanes = pl.ds(pl.multiple_of(((kv & 1) ^ which) * half, LANES), half)
        for s in range(steps):
            total = own_ref[s, :, lanes] + got_ref[0, s, :, lanes].astype(F32)
            total = total + came_ref[s, :, lanes].astype(F32)
            late = jnp.where(here, ref[s].astype(F32), 0.0)
            out_ref[s, :, lanes] = (total + late).astype(BF16)


def swap(values, axis, mask):
    pairs = [(i, i ^ mask) for i in range(lax.axis_size(axis))]
    return lax.ppermute(values, axis, pairs)


def local(
    queries,
    routes,
    suffix_lengths,
    prefix_keys,
    prefix_values,
    suffix_keys,
    suffix_values,
    new_keys,
    new_values,
    out_weight,
):
    owners, parts = lax.axis_size("dp"), lax.axis_size("kv")
    count, steps, width = queries.shape
    kv_width = prefix_keys.shape[2]
    heads = kv_width // HD
    group = width // kv_width
    capacity = max(2, 2 * count // owners)
    direct = owners == parts == 4 and capacity % 8 == 0
    blocks = owners if direct else 1
    size = capacity if direct else owners * capacity
    vmem, hbm = pl.BlockSpec(memory_space=pltpu.VMEM), pl.BlockSpec(memory_space=pltpu.HBM)
    far = lambda values: pltpu.with_memory_space_constraint(values, pltpu.HBM)
    names = routes.reshape(count)

    q, choice, *packed = pl.pallas_call(
        functools.partial(pack_kernel, capacity, direct),
        out_shape=[
            jax.ShapeDtypeStruct((steps, count, width), BF16),
            jax.ShapeDtypeStruct((count, owners * capacity), BF16),
        ]
        + [jax.ShapeDtypeStruct((steps, size, width), BF16)] * blocks,
        in_specs=[hbm, hbm],
        out_specs=[vmem] * (blocks + 2),
        scratch_shapes=[pltpu.SMEM((count,), jnp.int32), pltpu.SemaphoreType.DMA((2,))],
        compiler_params=params(8),
        cost_estimate=cost(2 * steps * owners * capacity * count * width, 1 << 20),
        name="pack",
    )(far(names), far(queries.transpose(1, 0, 2)))

    def all_to_all(values):
        values = values.reshape(steps, owners, capacity, -1)
        moved = lax.all_to_all(values, "dp", split_axis=1, concat_axis=1, tiled=True)
        return moved.reshape(steps, owners * capacity, -1)

    if direct:
        received = [packed[0]] + [swap(packed[i], "dp", i) for i in (1, 2, 3)]
    else:
        received = [all_to_all(packed[0])]

    rows = count * steps * group
    cached = suffix_keys.shape[1]
    new_shape = (steps, count, kv_width)
    keys, values = pl.pallas_call(
        load_kernel,
        out_shape=[jax.ShapeDtypeStruct(prefix_keys.shape[1:], BF16)] * 2,
        in_specs=[hbm] * 2,
        out_specs=[vmem] * 2,
        scratch_shapes=[pltpu.SemaphoreType.DMA((2 * PIECES,))],
        compiler_params=params(4),
        cost_estimate=cost(500_000_000, prefix_keys.size * 4),
        name="load",
    )(far(prefix_keys[0]), far(prefix_values[0]))
    own_rows, own_logs = pl.pallas_call(
        functools.partial(suffix_kernel, group),
        out_shape=[jax.ShapeDtypeStruct((steps, count, width), F32)] * 2,
        in_specs=[vmem] + [hbm] * 5,
        out_specs=[vmem] * 2,
        scratch_shapes=[
            pltpu.SMEM((count,), jnp.int32),
            pltpu.VMEM(suffix_keys.shape, BF16),
            pltpu.VMEM(suffix_keys.shape, BF16),
            pltpu.VMEM(new_shape, BF16),
            pltpu.VMEM(new_shape, BF16),
            pltpu.VMEM((heads * rows, HD), F32),
            pltpu.VMEM((rows, cached), F32),
            pltpu.VMEM((rows, cached), BF16),
            pltpu.VMEM((rows, HD), F32),
            pltpu.VMEM((rows, LANES), F32),
            pltpu.SemaphoreType.DMA((5,)),
        ],
        compiler_params=params(16),
        cost_estimate=cost(3_000_000_000, suffix_keys.size * 4, rows * 512),
        name="suffix",
    )(
        q,
        far(suffix_lengths),
        far(suffix_keys),
        far(suffix_values),
        far(new_keys.transpose(1, 0, 2)),
        far(new_values.transpose(1, 0, 2)),
    )

    prompt = pl.pallas_call(
        functools.partial(prompt_kernel, group),
        out_shape=jax.ShapeDtypeStruct((steps, size, width + LANES), BF16),
        in_specs=[vmem] * 3,
        out_specs=vmem,
        compiler_params=params(12 if direct else 48),
        cost_estimate=cost(4 * size * steps * width * prefix_keys.shape[1], prefix_keys.size * 4),
        name="prompt",
    )
    answers = []
    for asked in received:
        answers.append(prompt(asked, keys, values))
    if direct:
        home = [answers[0]] + [swap(answers[i], "dp", i) for i in (1, 2, 3)]
    else:
        home = [all_to_all(answers[0])]

    attended = pl.pallas_call(
        functools.partial(merge_kernel, blocks),
        out_shape=jax.ShapeDtypeStruct((steps, count, width), BF16),
        in_specs=[vmem] * (blocks + 3),
        out_specs=vmem,
        compiler_params=params(8),
        cost_estimate=cost(2 * steps * owners * capacity * count * width, 2 << 20),
        name="merge",
    )(choice, *home, own_rows, own_logs)

    columns = out_weight.shape[1]
    if not direct:
        block_rows = lax.all_gather(attended, "dp", axis=1, tiled=True)
        product = jnp.dot(
            block_rows.reshape(-1, width), out_weight, preferred_element_type=F32
        ).reshape(steps, -1, columns)
        total = lax.psum_scatter(product, "kv", scatter_dimension=1, tiled=True)
        return total.astype(BF16).transpose(1, 0, 2)

    by_two = swap(attended, "dp", 2)
    by_one = swap(attended, "dp", 1)
    by_three = swap(by_two, "dp", 1)
    half = columns // 2
    piece, halved = (steps, count, columns), (steps, count, half)
    flops = 2 * steps * count * width * columns

    def call(kernel, shapes, operands, scratch=(), work=1 << 20):
        return pl.pallas_call(
            kernel,
            out_shape=[jax.ShapeDtypeStruct(shape, kind) for shape, kind in shapes],
            in_specs=[vmem] * len(operands),
            out_specs=[vmem] * len(shapes),
            scratch_shapes=list(scratch),
            compiler_params=params(8),
            cost_estimate=cost(work, 1 << 20),
        )(*operands)

    own_sum, far_sum, beside = call(
        early_kernel,
        [(piece, F32), (piece, F32), ((2, *piece), BF16)],
        (attended, by_one, by_two, out_weight),
        [pltpu.VMEM((owners, steps * count, width), BF16)],
        4 * flops,
    )
    got = swap(beside, "kv", 1)
    (sent,) = call(add_kernel, [(piece, BF16)], (far_sum, got))
    came = swap(sent, "kv", 2)
    keep, send = call(
        late_kernel,
        [(halved, F32), (halved, BF16)],
        (by_three, out_weight),
        [pltpu.VMEM((steps * count, width), BF16)],
        flops,
    )
    sums = [(halved, F32), (halved, BF16)]
    keep, send = call(late_add_kernel, sums, (keep, swap(send, "kv", 1)))
    keep, send = call(late_add_kernel, sums, (keep, swap(send, "kv", 2)))
    other = swap(send, "kv", 1)
    (total,) = call(total_kernel, [(piece, BF16)], (own_sum, got, came, keep, other))
    return total.transpose(1, 0, 2)


def solution(mesh):
    placed = (
        P(("groups", "dp"), None, "kv"),
        P(("groups", "dp"), None),
        P(("groups", "dp")),
        P(("groups", "dp"), None, "kv"),
        P(("groups", "dp"), None, "kv"),
        P(("groups", "dp"), None, "kv"),
        P(("groups", "dp"), None, "kv"),
        P(("groups", "dp"), None, "kv"),
        P(("groups", "dp"), None, "kv"),
        P("kv", "dp"),
    )
    return jax.shard_map(
        local,
        mesh=mesh,
        in_specs=placed,
        out_specs=P(("groups", "kv"), None, "dp"),
        check_vma=False,
    )
```

```python
import functools
import math

import jax
import jax.numpy as jnp
from jax import lax
from jax.experimental import pallas as pl
from jax.experimental.pallas import tpu as pltpu
from jax.sharding import PartitionSpec as P


HD = 128
LANES = 128
F32 = jnp.float32
BF16 = jnp.bfloat16
HIDDEN = -1e30
MIB = 1 << 20
PIECES = 4
NT = (((1,), (1,)), ((), ()))


def params(mib):
    return pltpu.CompilerParams(vmem_limit_bytes=mib * MIB)


def cost(flops, nbytes, exps=0):
    return pl.CostEstimate(flops=flops, bytes_accessed=nbytes, transcendentals=exps)


def slots(routes_ref, count, capacity, base):
    names = [routes_ref[c] for c in range(count)]
    found = []
    for c in range(count):
        rank = jnp.int32(0)
        for earlier in range(c):
            rank = rank + (names[earlier] == names[c]).astype(jnp.int32)
        found.append((names[c] ^ base) * capacity + rank)
    return found


def spread(scalars, shape, dim):
    index = lax.broadcasted_iota(jnp.int32, shape, dim)
    out = jnp.full(shape, -1, jnp.int32)
    for c, value in enumerate(scalars):
        out = jnp.where(index == c, value, out)
    return out


def pack_kernel(capacity, relative, routes_ref, q_ref, held_ref, choice_ref, *refs):
    out_refs, (names, sems) = refs[:-2], refs[-2:]
    steps, count, _ = q_ref.shape
    name_copy = pltpu.make_async_copy(routes_ref, names, sems.at[0])
    q_copy = pltpu.make_async_copy(q_ref, held_ref, sems.at[1])
    name_copy.start()
    q_copy.start()
    base = lax.axis_index("dp") if relative else 0
    name_copy.wait()
    found = slots(names, count, capacity, base)
    shape = choice_ref.shape
    choice = spread(found, shape, 0) == lax.broadcasted_iota(jnp.int32, shape, 1)
    choice_ref[...] = choice.astype(BF16)
    shape = shape[::-1]
    placement = (spread(found, shape, 1) == lax.broadcasted_iota(jnp.int32, shape, 0)).astype(BF16)
    q_copy.wait()
    for s in range(steps):
        rows = jnp.dot(placement, held_ref[s], preferred_element_type=F32)
        at = 0
        for ref in out_refs:
            ref[s] = rows[at : at + ref.shape[1]].astype(BF16)
            at += ref.shape[1]


def suffix_kernel(
    group,
    q_ref,
    len_hbm,
    k_hbm,
    v_hbm,
    nk_hbm,
    nv_hbm,
    o_ref,
    l_ref,
    len_ref,
    k_ref,
    v_ref,
    nk_ref,
    nv_ref,
    qs,
    ss,
    ps,
    os,
    ls,
    sems,
):
    pairs = (
        (len_hbm, len_ref),
        (k_hbm, k_ref),
        (nk_hbm, nk_ref),
        (nv_hbm, nv_ref),
        (v_hbm, v_ref),
    )
    copies = [
        pltpu.make_async_copy(source, target, sems.at[i])
        for i, (source, target) in enumerate(pairs)
    ]
    for copy in copies:
        copy.start()
    steps, count, width = q_ref.shape
    heads = width // HD // group
    cached = k_ref.shape[1]
    each = steps * group
    rows = count * each
    scale = 1.0 / math.sqrt(HD)
    to_two = scale * math.log2(math.e)
    for h in range(heads):
        for s in range(steps):
            for g in range(group):
                piece = q_ref[s, :, pl.ds((h * group + g) * HD, HD)].astype(F32)
                qs[pl.ds(h * rows + s * group + g, count, stride=each), :] = piece
    row = lax.broadcasted_iota(jnp.int32, (rows, steps * count), 0).astype(F32)
    column = lax.broadcasted_iota(jnp.int32, (rows, steps * count), 1).astype(F32)
    row_cand = jnp.floor((row + 0.5) * (1.0 / each))
    row_step = jnp.floor((row - row_cand * each + 0.5) * (1.0 / group))
    key_step = jnp.floor((column + 0.5) * (1.0 / count))
    key_cand = column - key_step * count
    visible = (row_cand == key_cand) & (key_step <= row_step)
    position = lax.broadcasted_iota(jnp.int32, (each, cached), 1)
    for copy in copies[:4]:
        copy.wait()
    for h in range(heads):
        for c in range(count):
            qc = qs[pl.ds(h * rows + c * each, each), :].astype(BF16)
            kc = k_ref[c, :, pl.ds(h * HD, HD)]
            score = lax.dot_general(qc, kc, NT, preferred_element_type=F32)
            ss[pl.ds(c * each, each), :] = jnp.where(position < len_ref[c], score, HIDDEN)
        nk = jnp.concatenate([nk_ref[t, :, pl.ds(h * HD, HD)] for t in range(steps)], 0)
        nv = jnp.concatenate([nv_ref[t, :, pl.ds(h * HD, HD)] for t in range(steps)], 0)
        fresh = lax.dot_general(
            qs[pl.ds(h * rows, rows), :].astype(BF16), nk, NT, preferred_element_type=F32
        )
        fresh = jnp.where(visible, fresh, HIDDEN)
        score = ss[...]
        peak = jnp.maximum(
            jnp.max(score, -1, keepdims=True), jnp.max(fresh, -1, keepdims=True)
        )
        weight = jnp.exp2((score - peak) * to_two)
        fresh = jnp.exp2((fresh - peak) * to_two)
        total = jnp.sum(weight, -1, keepdims=True) + jnp.sum(fresh, -1, keepdims=True)
        ps[...] = weight.astype(BF16)
        if h == 0:
            copies[4].wait()
        os[...] = jnp.dot(fresh.astype(BF16), nv, preferred_element_type=F32)
        for c in range(count):
            vc = v_ref[c, :, pl.ds(h * HD, HD)]
            pc = ps[pl.ds(c * each, each), :]
            os[pl.ds(c * each, each), :] += jnp.dot(pc, vc, preferred_element_type=F32)
        os[...] = os[...] / total
        ls[...] = jnp.broadcast_to(peak * scale + jnp.log(total), ls.shape)
        for s in range(steps):
            for g in range(group):
                at = pl.ds(s * group + g, count, stride=each)
                lanes = pl.ds((h * group + g) * HD, HD)
                o_ref[s, :, lanes] = os[at, :]
                l_ref[s, :, lanes] = ls[at, :]


def load_kernel(k_hbm, v_hbm, k_ref, v_ref, sems):
    copies = []
    for source, target in ((k_hbm, k_ref), (v_hbm, v_ref)):
        part = source.shape[0] // PIECES
        for at in range(0, source.shape[0], part):
            pair = source.at[pl.ds(at, part)], target.at[pl.ds(at, part)]
            copies.append(pltpu.make_async_copy(*pair, sems.at[len(copies)]))
    for copy in copies:
        copy.start()
    for copy in copies:
        copy.wait()


def prompt_kernel(group, q_ref, k_ref, v_ref, out_ref):
    steps, size, width = q_ref.shape
    heads = width // HD // group
    all_heads = heads * group
    scale = 1.0 / math.sqrt(HD)
    to_two = scale * math.log2(math.e)
    lane = lax.broadcasted_iota(jnp.int32, (size, LANES), 1)
    place = lax.rem(lane, all_heads) + lax.div(lane, 2 * all_heads) * all_heads
    logs = jnp.zeros((size, LANES), F32)
    scores = []
    for h in range(heads):
        q = jnp.concatenate(
            [
                q_ref[s, :, pl.ds((h * group + g) * HD, HD)]
                for s in range(steps)
                for g in range(group)
            ],
            0,
        )
        keys = k_ref[:, pl.ds(h * HD, HD)]
        scores.append(lax.dot_general(q, keys, NT, preferred_element_type=F32))
    for h in range(heads):
        values = v_ref[:, pl.ds(h * HD, HD)]
        score = scores[h]
        peak = jnp.max(score, -1, keepdims=True)
        weight = jnp.exp2((score - peak) * to_two)
        total = jnp.sum(weight, -1, keepdims=True)
        out = jnp.dot(weight.astype(BF16), values, preferred_element_type=F32) / total
        log_total = peak * scale + jnp.log(total)
        for s in range(steps):
            for g in range(group):
                at = (s * group + g) * size
                head = s * all_heads + h * group + g
                out_ref[:, pl.ds(head * HD, HD)] = out[at : at + size].astype(BF16)
                logs = jnp.where(place == head, log_total[at : at + size], logs)
    high = logs.astype(BF16).astype(F32)
    terms = jnp.where(lax.rem(lane, 2 * all_heads) < all_heads, high, logs - high)
    out_ref[:, pl.ds(steps * width, LANES)] = terms.astype(BF16)


def merge_kernel(blocks, *refs):
    choice_ref, row_refs = refs[0], refs[1 : 1 + blocks]
    own_ref, log_ref, out_ref = refs[1 + blocks :]
    steps, count, width = own_ref.shape
    all_heads = width // HD
    choice = choice_ref[...]
    received = jnp.concatenate([ref[...] for ref in row_refs], 0)
    received = jnp.dot(choice, received, preferred_element_type=F32)
    for s in range(steps):
        rows = received[:, s * width : (s + 1) * width]
        at = steps * width + 2 * s * all_heads
        logs = received[:, at : at + all_heads] + received[:, at + all_heads : at + 2 * all_heads]
        for h in range(all_heads):
            lanes = slice(h * HD, (h + 1) * HD)
            first = jnp.broadcast_to(logs[:, h : h + 1], (count, HD))
            second = log_ref[s, :, lanes]
            peak = jnp.maximum(first, second)
            first = jnp.exp(first - peak)
            second = jnp.exp(second - peak)
            mixed = (first * rows[:, lanes] + second * own_ref[s, :, lanes]) / (first + second)
            out_ref[s, :, lanes] = mixed.astype(BF16)


CHUNK = 512


def early_kernel(own_ref, g1_ref, g2_ref, w_ref, own_out, far_out, beside_out, held):
    steps, count, _ = own_ref.shape
    each = steps * count
    me, mine = lax.axis_index("dp"), lax.axis_index("kv")
    for shift, ref in enumerate((own_ref, g1_ref, g2_ref)):
        place = (me ^ shift) ^ mine
        for s in range(steps):
            held[place, pl.ds(s * count, count), :] = ref[s]
    held[(me ^ 3) ^ mine, :, :] = jnp.zeros(held.shape[1:], BF16)
    rows = held[...].reshape(4 * each, held.shape[2])
    outs = (own_out, beside_out.at[0], far_out, beside_out.at[1])
    for at in range(0, w_ref.shape[1], CHUNK):
        lanes = pl.ds(at, CHUNK)
        product = jnp.dot(rows, w_ref[:, lanes], preferred_element_type=F32)
        for part, ref in enumerate(outs):
            for s in range(steps):
                row = part * each + s * count
                ref[s, :, lanes] = product[row : row + count].astype(ref.dtype)


def late_kernel(rows_ref, w_ref, keep_out, send_out, held):
    steps, count, half = keep_out.shape
    core = lax.axis_index("kv") & 1
    for s in range(steps):
        held[pl.ds(s * count, count), :] = rows_ref[s]
    for which, ref in ((1, send_out), (0, keep_out)):
        for at in range(0, half, CHUNK):
            first = pl.multiple_of((core ^ which) * half + at, CHUNK)
            product = jnp.dot(held[...], w_ref[:, pl.ds(first, CHUNK)], preferred_element_type=F32)
            for s in range(steps):
                ref[s, :, pl.ds(at, CHUNK)] = product[s * count : (s + 1) * count].astype(ref.dtype)


def add_kernel(keep_ref, got_ref, send_ref):
    for s in range(keep_ref.shape[0]):
        send_ref[s] = (keep_ref[s] + got_ref[1, s].astype(F32)).astype(BF16)


def late_add_kernel(keep_ref, got_ref, sum_ref, send_ref):
    for s in range(keep_ref.shape[0]):
        total = keep_ref[s] + got_ref[s].astype(F32)
        sum_ref[s] = total
        send_ref[s] = total.astype(BF16)


def total_kernel(own_ref, got_ref, came_ref, half_ref, other_ref, out_ref):
    steps, _, half = half_ref.shape
    kv = lax.axis_index("kv")
    here = kv == (lax.axis_index("dp") ^ 3)
    for which, ref in ((0, half_ref), (1, other_ref)):
        lanes = pl.ds(pl.multiple_of(((kv & 1) ^ which) * half, LANES), half)
        for s in range(steps):
            total = own_ref[s, :, lanes] + got_ref[0, s, :, lanes].astype(F32)
            total = total + came_ref[s, :, lanes].astype(F32)
            late = jnp.where(here, ref[s].astype(F32), 0.0)
            out_ref[s, :, lanes] = (total + late).astype(BF16)


def swap(values, axis, mask):
    pairs = [(i, i ^ mask) for i in range(lax.axis_size(axis))]
    return lax.ppermute(values, axis, pairs)


def local(
    queries,
    routes,
    suffix_lengths,
    prefix_keys,
    prefix_values,
    suffix_keys,
    suffix_values,
    new_keys,
    new_values,
    out_weight,
):
    owners, parts = lax.axis_size("dp"), lax.axis_size("kv")
    count, steps, width = queries.shape
    kv_width = prefix_keys.shape[2]
    heads = kv_width // HD
    group = width // kv_width
    capacity = max(2, 2 * count // owners)
    direct = owners == parts == 4 and capacity % 8 == 0
    blocks = owners if direct else 1
    size = capacity if direct else owners * capacity
    vmem, hbm = pl.BlockSpec(memory_space=pltpu.VMEM), pl.BlockSpec(memory_space=pltpu.HBM)
    far = lambda values: pltpu.with_memory_space_constraint(values, pltpu.HBM)
    names = routes.reshape(count)

    q, choice, *packed = pl.pallas_call(
        functools.partial(pack_kernel, capacity, direct),
        out_shape=[
            jax.ShapeDtypeStruct((steps, count, width), BF16),
            jax.ShapeDtypeStruct((count, owners * capacity), BF16),
        ]
        + [jax.ShapeDtypeStruct((steps, size, width), BF16)] * blocks,
        in_specs=[hbm, hbm],
        out_specs=[vmem] * (blocks + 2),
        scratch_shapes=[pltpu.SMEM((count,), jnp.int32), pltpu.SemaphoreType.DMA((2,))],
        compiler_params=params(8),
        cost_estimate=cost(2 * steps * owners * capacity * count * width, 1 << 20),
        name="pack",
    )(far(names), far(queries.transpose(1, 0, 2)))

    def all_to_all(values):
        values = values.reshape(steps, owners, capacity, -1)
        moved = lax.all_to_all(values, "dp", split_axis=1, concat_axis=1, tiled=True)
        return moved.reshape(steps, owners * capacity, -1)

    if direct:
        received = [packed[0]] + [swap(packed[i], "dp", i) for i in (1, 2, 3)]
    else:
        received = [all_to_all(packed[0])]

    rows = count * steps * group
    cached = suffix_keys.shape[1]
    new_shape = (steps, count, kv_width)
    keys, values = pl.pallas_call(
        load_kernel,
        out_shape=[jax.ShapeDtypeStruct(prefix_keys.shape[1:], BF16)] * 2,
        in_specs=[hbm] * 2,
        out_specs=[vmem] * 2,
        scratch_shapes=[pltpu.SemaphoreType.DMA((2 * PIECES,))],
        compiler_params=params(4),
        cost_estimate=cost(500_000_000, prefix_keys.size * 4),
        name="load",
    )(far(prefix_keys[0]), far(prefix_values[0]))
    own_rows, own_logs = pl.pallas_call(
        functools.partial(suffix_kernel, group),
        out_shape=[jax.ShapeDtypeStruct((steps, count, width), F32)] * 2,
        in_specs=[vmem] + [hbm] * 5,
        out_specs=[vmem] * 2,
        scratch_shapes=[
            pltpu.SMEM((count,), jnp.int32),
            pltpu.VMEM(suffix_keys.shape, BF16),
            pltpu.VMEM(suffix_keys.shape, BF16),
            pltpu.VMEM(new_shape, BF16),
            pltpu.VMEM(new_shape, BF16),
            pltpu.VMEM((heads * rows, HD), F32),
            pltpu.VMEM((rows, cached), F32),
            pltpu.VMEM((rows, cached), BF16),
            pltpu.VMEM((rows, HD), F32),
            pltpu.VMEM((rows, LANES), F32),
            pltpu.SemaphoreType.DMA((5,)),
        ],
        compiler_params=params(16),
        cost_estimate=cost(3_000_000_000, suffix_keys.size * 4, rows * 512),
        name="suffix",
    )(
        q,
        far(suffix_lengths),
        far(suffix_keys),
        far(suffix_values),
        far(new_keys.transpose(1, 0, 2)),
        far(new_values.transpose(1, 0, 2)),
    )

    prompt = pl.pallas_call(
        functools.partial(prompt_kernel, group),
        out_shape=jax.ShapeDtypeStruct((size, steps * width + LANES), BF16),
        in_specs=[vmem] * 3,
        out_specs=vmem,
        compiler_params=params(12 if direct else 48),
        cost_estimate=cost(4 * size * steps * width * prefix_keys.shape[1], prefix_keys.size * 4),
        name="prompt",
    )
    answers = []
    for asked in received:
        answers.append(prompt(asked, keys, values))
    if direct:
        home = [answers[0]] + [swap(answers[i], "dp", i) for i in (1, 2, 3)]
    else:
        moved = answers[0].reshape(owners, capacity, -1)
        moved = lax.all_to_all(moved, "dp", split_axis=0, concat_axis=0, tiled=True)
        home = [moved.reshape(owners * capacity, -1)]

    attended = pl.pallas_call(
        functools.partial(merge_kernel, blocks),
        out_shape=jax.ShapeDtypeStruct((steps, count, width), BF16),
        in_specs=[vmem] * (blocks + 3),
        out_specs=vmem,
        compiler_params=params(8),
        cost_estimate=cost(2 * steps * owners * capacity * count * width, 2 << 20),
        name="merge",
    )(choice, *home, own_rows, own_logs)

    columns = out_weight.shape[1]
    if not direct:
        block_rows = lax.all_gather(attended, "dp", axis=1, tiled=True)
        product = jnp.dot(
            block_rows.reshape(-1, width), out_weight, preferred_element_type=F32
        ).reshape(steps, -1, columns)
        total = lax.psum_scatter(product, "kv", scatter_dimension=1, tiled=True)
        return total.astype(BF16).transpose(1, 0, 2)

    by_two = swap(attended, "dp", 2)
    by_one = swap(attended, "dp", 1)
    by_three = swap(by_two, "dp", 1)
    half = columns // 2
    piece, halved = (steps, count, columns), (steps, count, half)
    flops = 2 * steps * count * width * columns

    def call(kernel, shapes, operands, scratch=(), work=1 << 20):
        return pl.pallas_call(
            kernel,
            out_shape=[jax.ShapeDtypeStruct(shape, kind) for shape, kind in shapes],
            in_specs=[vmem] * len(operands),
            out_specs=[vmem] * len(shapes),
            scratch_shapes=list(scratch),
            compiler_params=params(8),
            cost_estimate=cost(work, 1 << 20),
        )(*operands)

    own_sum, far_sum, beside = call(
        early_kernel,
        [(piece, F32), (piece, F32), ((2, *piece), BF16)],
        (attended, by_one, by_two, out_weight),
        [pltpu.VMEM((owners, steps * count, width), BF16)],
        4 * flops,
    )
    got = swap(beside, "kv", 1)
    (sent,) = call(add_kernel, [(piece, BF16)], (far_sum, got))
    came = swap(sent, "kv", 2)
    keep, send = call(
        late_kernel,
        [(halved, F32), (halved, BF16)],
        (by_three, out_weight),
        [pltpu.VMEM((steps * count, width), BF16)],
        flops,
    )
    sums = [(halved, F32), (halved, BF16)]
    keep, send = call(late_add_kernel, sums, (keep, swap(send, "kv", 1)))
    keep, send = call(late_add_kernel, sums, (keep, swap(send, "kv", 2)))
    other = swap(send, "kv", 1)
    (total,) = call(total_kernel, [(piece, BF16)], (own_sum, got, came, keep, other))
    return total.transpose(1, 0, 2)


def solution(mesh):
    placed = (
        P(("groups", "dp"), None, "kv"),
        P(("groups", "dp"), None),
        P(("groups", "dp")),
        P(("groups", "dp"), None, "kv"),
        P(("groups", "dp"), None, "kv"),
        P(("groups", "dp"), None, "kv"),
        P(("groups", "dp"), None, "kv"),
        P(("groups", "dp"), None, "kv"),
        P(("groups", "dp"), None, "kv"),
        P("kv", "dp"),
    )
    return jax.shard_map(
        local,
        mesh=mesh,
        in_specs=placed,
        out_specs=P(("groups", "kv"), None, "dp"),
        check_vma=False,
    )
```
